128 devices in a mesh: prow: 8 (over y, core), pcol: 16 (over z, x).
Axes of the slice: x: 4, y: 4, z: 4, core: 2. Of those that a mesh axis runs over, the one named last changes fastest.
Arguments:
- inverse_cov: bfloat16 [8192, 8192], P('prow', 'pcol'), may hold values from -0.5 to 4.5, as said below
- cosines: float32 [8192, 8192], P('prow', 'pcol'), may hold values from -1 to 1, as said below
- sky_maps: bfloat16 [8192, 192], P('pcol'), may hold values from -6 to 6
Outputs:
- filtered: bfloat16 [8192, 192], P('prow')
- spectra: float32 [64, 192], replicated
The draws below stay inside these ranges and needn't reach their ends.
Inputs may be any that keep to these rules, and one draw needn't show every extreme that they name: `inverse_cov`: symmetric, with a dominant diagonal. `cosines`: symmetric.
All inputs are finite; a program needn't handle non-finite values.
Results may differ from the reference program's by a relative error of at most 0.0033.
Values may be sent and summed in bfloat16 or wider, within the bound.
No kernel may reach another device: no remote copies, remote signals or barrier semaphores. Data moves between devices by JAX's collectives and lax.ppermute only.
A program may use at most 64 MiB of HBM per device.

```python
import math
import jax
import jax.numpy as jnp
from jax import lax

NPIX = 8192
MAPS = 192
L = 64
LMIN = 2


def draw_inverse_cov(key, part):
    first_key, second_key = jax.random.split(jax.random.fold_in(key, 11))
    noise = jax.random.truncated_normal(first_key, -6.0, 6.0, (NPIX, NPIX), jnp.float32) * (0.5 / math.sqrt(NPIX))
    symmetric = noise + noise.T
    diagonal = jax.random.uniform(second_key, (NPIX,), jnp.float32, 1.0, 2.0)
    return (symmetric + jnp.diag(diagonal)).astype(jnp.bfloat16)


def draw_cosines(key, part):
    vector_key, rough_key = jax.random.split(jax.random.fold_in(key, 23))
    vectors = jax.random.normal(vector_key, (NPIX, 3), jnp.float32)
    rough = jax.random.truncated_normal(rough_key, -4.0, 4.0, (NPIX, NPIX), jnp.float32) * 0.05
    units = vectors / jnp.sqrt(jnp.sum(vectors * vectors, axis=1, keepdims=True) + 1e-12)
    product = jnp.dot(units, units.T, precision=lax.Precision.HIGHEST)
    return jnp.clip(product + rough + rough.T, -1.0, 1.0)


def shard_levels(rng, extent, pieces, smallest, high):
    level = 1.0
    for dim, shards_of in pieces:
        steps = jax.random.uniform(jax.random.fold_in(jax.random.fold_in(rng, 6), dim), (shards_of,), jnp.float32, smallest / len(pieces), high / len(pieces))
        level = level * jnp.repeat(jnp.exp(steps), extent[dim] // shards_of).reshape((-1,) + (1,) * (len(extent) - 1 - dim))
    return level


def normal_values(rng, shape, scale, limit, cuts=(), kind=jnp.bfloat16):
    values = scale * jax.random.normal(rng, shape, jnp.float32)
    if cuts:
        values = values * shard_levels(rng, shape, cuts, -0.22, 0.18)
    return jnp.clip(values, -limit, limit).astype(kind)


def setup_inputs(seed: int = 0) -> dict:
    streams_of = jax.random.split(jax.random.key(seed), 4)
    inverse_cov = draw_inverse_cov(jax.random.fold_in(streams_of[3], 71), 0)
    cosines = draw_cosines(jax.random.fold_in(streams_of[3], 71), 0)
    sky_maps = normal_values(streams_of[2], (NPIX, MAPS), 1.0, 6.0, ((0, 16),))
    return {"inverse_cov": inverse_cov, "cosines": cosines, "sky_maps": sky_maps}


def next_legendre(previous, current, cosine, degree):
    return ((2.0 * degree - 1.0) * cosine * current - (degree - 1.0) * previous) / degree


def reference(inverse_cov, cosines, sky_maps):
    filtered = jnp.dot(inverse_cov, sky_maps, preferred_element_type=jnp.float32).astype(jnp.bfloat16)
    maps_f32 = filtered.astype(jnp.float32)
    blocks = 8
    size_rows = NPIX // blocks
    degrees = (jnp.arange(L) + LMIN).astype(jnp.float32)

    def block_spectra(block_index):
        first_row = (block_index * size_rows).astype(jnp.int32)
        cosine = lax.dynamic_slice_in_dim(cosines, first_row, size_rows, 0)
        rows_f32 = lax.dynamic_slice_in_dim(maps_f32, first_row, size_rows, 0)
        previous = jnp.ones_like(cosine)
        current = cosine
        for low_degree in range(2, LMIN):
            next_term = next_legendre(previous, current, cosine, jnp.float32(low_degree))
            previous, current = current, next_term

        def advance(carried, degree):
            previous, current = carried
            next_term = next_legendre(previous, current, cosine, degree)
            product = jnp.dot(next_term.astype(jnp.bfloat16), filtered, preferred_element_type=jnp.float32)
            spectrum = jnp.sum(rows_f32 * product, axis=0) * ((2.0 * degree + 1.0) / NPIX)
            return (current, next_term), spectrum

        carried, values = lax.scan(advance, (previous, current), degrees)
        return values

    per_block = lax.map(block_spectra, jnp.arange(blocks, dtype=jnp.int32))
    return filtered, jnp.sum(per_block, axis=0)
```

```python
import functools

import jax
import jax.numpy as jnp
import numpy as np
from jax import lax
from jax.experimental import pallas as pl
from jax.experimental.pallas import tpu as pltpu
from jax.sharding import Mesh
from jax.sharding import PartitionSpec as P

NPIX = 8192
MAPS = 192
L = 64
LMIN = 2
TOP = LMIN + L - 1
NR, NC = 8, 16
CHUNK = NPIX // NC
PIECE = CHUNK // NR
LANES = 256
ROWS = 32
COLS = 256
PROW = ("prow_0", "prow_1")
PCOL = ("pcol_0", "pcol_1")
ALL = PROW + PCOL
bf16, f32 = jnp.bfloat16, jnp.float32


def half_of(r, c):
    if c // 2 == r:
        return 1 - c % 2
    return c % 2 if c // 2 > r else 1 - c % 2


HALF = np.array([[half_of(r, c) for c in range(NC)] for r in range(NR)])
MEMBERS = [[[c for c in range(NC) if HALF[r, c] == s] for s in range(2)] for r in range(NR)]
PIECE_OF = np.array(
    [[8 * HALF[r, c] + MEMBERS[r][HALF[r, c]].index(c) for c in range(NC)] for r in range(NR)]
)
ROW_GROUPS = [[r * NC + c for c in MEMBERS[r][s]] for r in range(NR) for s in range(2)]
TO_COLUMNS = [
    (r * NC + MEMBERS[r][s][j], j * NC + 2 * r + s)
    for r in range(NR) for s in range(2) for j in range(NR)
]
OTHER_HALF = [
    (r * NC + MEMBERS[r][s][j], r * NC + MEMBERS[r][1 - s][j])
    for r in range(NR) for s in range(2) for j in range(NR)
]


def tile_tables():
    plans = []
    for s in range(2):
        plans.append(
            [(512 * s + 32 * u, 32 * u, h, 1) for h in range(2) for u in range(16)]
        )
    for own in range(2):
        other = 1 - own
        mine, theirs = 512 * own, 512 * other
        tiles = [(mine + 32 * u, 512 + 32 * u, 0, 0) for u in range(8)]
        tiles += [(mine + 32 * u, 512 + 32 * u, 1, 1) for u in range(8)]
        tiles += [(mine + 256 + 32 * u, 768 + 32 * u, 1, 0) for u in range(8)]
        if own == 0:
            tiles += [(theirs + 32 * u, 32 * u, h, 1) for h in range(2) for u in range(8)]
        else:
            tiles += [(theirs + 32 * u, 32 * u, 1, 1) for u in range(16)]
        plans.append(tiles)
    most = max(map(len, plans)) + 2
    table = np.zeros((4, most, 4), np.int32)
    counts = np.zeros((4,), np.int32)
    for kind, tiles in enumerate(plans):
        counts[kind] = len(tiles)
        table[kind] = np.array(tiles + [tiles[-1]] * (most - len(tiles)))
    return table, counts


TABLE, COUNTS = tile_tables()


def basis_matrix():
    g = [1.0]
    for k in range(1, TOP + 1):
        g.append(g[-1] * (2 * k - 1) / (2 * k))
    matrix = np.zeros((L, TOP + 1))
    for row in range(L):
        degree = row + LMIN
        for k in range(degree + 1):
            matrix[row, abs(degree - 2 * k)] += g[k] * g[degree - k]
        matrix[row] *= 2.0 * (2.0 * degree + 1.0) / NPIX
    return np.repeat(matrix, 8, axis=1).astype(np.float32)


BASIS = basis_matrix()


def partial_kernel(order_ref, cov_ref, maps_ref, out_ref):
    product = jnp.dot(cov_ref[...], maps_ref[...], preferred_element_type=f32)
    for piece in range(NC):
        rows = product[PIECE * piece : PIECE * (piece + 1)]
        out_ref[order_ref[piece]] = rows.astype(bf16)


def spectra_kernel(
    kind_ref, counts_ref, table_ref, cos_ref, rows_ref, cols_ref, basis_ref, out_ref,
    maps, weights, even, odd, total,
):
    kind = kind_ref[0]
    zeros = jnp.zeros((CHUNK, LANES - MAPS), bf16)
    col_maps = jnp.concatenate([cols_ref[...], zeros], axis=1)
    row_maps = jnp.concatenate([rows_ref[...], zeros], axis=1)
    weights[0] = col_maps[:COLS]
    weights[1] = col_maps[COLS:]
    maps[:CHUNK] = row_maps
    maps[CHUNK:] = col_maps
    row_sum = jnp.sum(row_maps.astype(f32), axis=0, keepdims=True)
    col_sum = jnp.sum(col_maps.astype(f32), axis=0, keepdims=True)
    diagonal = kind >= 2
    alpha = jnp.where(diagonal, 0.5, 1.0)
    beta = jnp.where(diagonal, 0.5, 0.0)
    total[...] = jnp.zeros_like(total)
    total[0, 0:1] = col_sum * (alpha * row_sum + beta * col_sum)

    def generate(t, slot):
        row = pl.multiple_of(table_ref[kind, t, 0], ROWS)
        col = pl.multiple_of(table_ref[kind, t, 2] * COLS, COLS)
        x = cos_ref[pl.ds(row, ROWS), pl.ds(col, COLS)]
        twice = x + x
        previous, current = jnp.ones_like(x), x
        slot[0] = x.astype(bf16)
        for k in range(2, TOP + 1):
            previous, current = current, twice * current - previous
            slot[k - 1] = current.astype(bf16)

    def contract(t, slot):
        row = pl.multiple_of(table_ref[kind, t, 1], ROWS)
        weight = jnp.where(table_ref[kind, t, 3] == 1, 1.0, 0.5)
        left = maps[pl.ds(row, ROWS)].astype(f32) * weight
        right = weights[table_ref[kind, t, 2]]
        image = jnp.dot(slot[...].reshape(TOP * ROWS, COLS), right, preferred_element_type=f32)
        for k in range(TOP):
            product = image[ROWS * k : ROWS * (k + 1)] * left
            total[k + 1] += jnp.sum(product.reshape(ROWS // 8, 8, LANES), axis=0)

    generate(0, even)

    def step(pair, carry):
        t = 2 * pair
        generate(t + 1, odd)
        contract(t, even)
        generate(t + 2, even)
        contract(t + 1, odd)
        return carry

    lax.fori_loop(0, counts_ref[kind] // 2, step, 0)
    sums = total[...].reshape((TOP + 1) * 8, LANES)
    out_ref[...] = jnp.dot(
        basis_ref[...], sums, preferred_element_type=f32, precision=lax.Precision.HIGHEST
    )


SMEM = pl.BlockSpec(memory_space=pltpu.SMEM)
VMEM = pl.BlockSpec(memory_space=pltpu.VMEM)


def partial_products(order, cov, maps):
    return pl.pallas_call(
        partial_kernel,
        out_shape=jax.ShapeDtypeStruct((NC, PIECE, MAPS), bf16),
        in_specs=[SMEM, VMEM, VMEM],
        out_specs=VMEM,
        name="partial",
    )(order, cov, maps)


def block_spectra(kind, cosines, rows, cols):
    return pl.pallas_call(
        spectra_kernel,
        out_shape=jax.ShapeDtypeStruct((L, LANES), f32),
        in_specs=[SMEM, SMEM, SMEM, VMEM, VMEM, VMEM, VMEM],
        out_specs=VMEM,
        scratch_shapes=[
            pltpu.VMEM((2 * CHUNK, LANES), bf16),
            pltpu.VMEM((2, COLS, LANES), bf16),
            pltpu.VMEM((TOP, ROWS, COLS), bf16),
            pltpu.VMEM((TOP, ROWS, COLS), bf16),
            pltpu.VMEM((TOP + 1, 8, LANES), f32),
        ],
        cost_estimate=pl.CostEstimate(flops=9 * 10**9, bytes_accessed=4 * 10**6, transcendentals=0),
        name="spectra",
    )(kind, jnp.asarray(COUNTS), jnp.asarray(TABLE), cosines, rows, cols, jnp.asarray(BASIS))


def from_everyone(value, axis, groups=None):
    length = NR
    copies = jnp.broadcast_to(value[None], (length, *value.shape))
    return lax.all_to_all(copies, axis, 0, 0, axis_index_groups=groups, tiled=True)


def everywhere(value):
    value = value + lax.ppermute(value, PROW[1], [(0, 1), (1, 0)])
    for axis in (PROW[0],) + PCOL:
        value = value + lax.ppermute(value, axis, [(0, 1), (1, 0), (2, 3), (3, 2)])
        value = value + lax.ppermute(value, axis, [(0, 3), (3, 0), (2, 1), (1, 2)])
    return value


def per_device(inverse_cov, cosines, sky_maps):
    r, c = lax.axis_index(PROW), lax.axis_index(PCOL)
    half = jnp.asarray(HALF, jnp.int32)[r, c]
    places = np.zeros((NR, NC), np.int32)
    for row in range(NR):
        places[row, PIECE_OF[row]] = np.arange(NC)
    order = jnp.asarray(places)[r]
    kind = jnp.where(c // 2 == r, 2 + c % 2, half).astype(jnp.int32).reshape(1)

    partial = partial_products(order, inverse_cov, sky_maps)
    parts = lax.all_to_all(partial, PCOL, 0, 0, tiled=True)
    piece = jnp.sum(parts.astype(f32), axis=0).astype(bf16)

    moved = lax.ppermute(piece, ALL, TO_COLUMNS)
    rows = from_everyone(piece, ALL, ROW_GROUPS).reshape(CHUNK, MAPS)
    other = lax.ppermute(rows, ALL, OTHER_HALF)
    cols = from_everyone(moved, PROW).reshape(CHUNK, MAPS)

    share = block_spectra(kind, cosines, rows, cols)
    spectra = everywhere(share[:, :MAPS])
    first = jnp.where(half == 0, rows, other)
    second = jnp.where(half == 0, other, rows)
    return jnp.concatenate([first, second], axis=0), spectra


def solution(mesh):
    split = Mesh(mesh.devices.reshape(4, 2, 4, 4), ALL)
    placed = (P(PROW, PCOL), P(PROW, PCOL), P(PCOL, None))
    return jax.shard_map(
        per_device, mesh=split, in_specs=placed, out_specs=(P(PROW, None), P()), check_vma=False
    )
```

```python
import functools

import jax
import jax.numpy as jnp
import numpy as np
from jax import lax
from jax.experimental import pallas as pl
from jax.experimental.pallas import tpu as pltpu
from jax.sharding import Mesh
from jax.sharding import PartitionSpec as P

NPIX = 8192
MAPS = 192
L = 64
LMIN = 2
TOP = LMIN + L - 1
NR, NC = 8, 16
CHUNK = NPIX // NC
PIECE = CHUNK // NR
LANES = 256
ROWS = 32
COLS = 256
LOW = 9
CENTRES = (18, 37, 56)
PROW = ("prow_0", "prow_1")
PCOL = ("pcol_0", "pcol_1")
ALL = PROW + PCOL
bf16, f16, f32 = jnp.bfloat16, jnp.float16, jnp.float32
MASKS = (1, 2, 6)
ORDER = (0, 1, 2, 3, 6, 7, 4, 5)


def half_of(r, c):
    return c % 2 if c // 2 > r else 1 - c % 2


MEMBERS = [
    [[c for c in range(NC) if half_of(r, c) == s] for s in range(2)] for r in range(NR)
]
EACH = [(r, s, g) for r in range(NR) for s in range(2) for g in range(NR)]
TO_COLUMNS = [(r * NC + MEMBERS[r][s][g], g * NC + 2 * r + s) for r, s, g in EACH]
OTHER_HALF = [(r * NC + MEMBERS[r][s][g], r * NC + MEMBERS[r][1 - s][g]) for r, s, g in EACH]
ROW_STEPS = [
    [(r * NC + MEMBERS[r][s][g], r * NC + MEMBERS[r][s][g ^ mask]) for r, s, g in EACH]
    for mask in MASKS
]
COLUMN_STEPS = [
    [(r * NC + c, (r ^ mask) * NC + c) for r in range(NR) for c in range(NC)] for mask in MASKS
]


def basis_matrix():
    g = [1.0]
    for k in range(1, TOP + 1):
        g.append(g[-1] * (2 * k - 1) / (2 * k))
    cheb = np.zeros((L, TOP + 1))
    for row in range(L):
        degree = row + LMIN
        for k in range(degree + 1):
            cheb[row, abs(degree - 2 * k)] += g[k] * g[degree - k]
        cheb[row] *= 2.0 * (2.0 * degree + 1.0) / NPIX
    columns = [cheb[:, k] for k in range(LOW)]
    for n in CENTRES:
        columns.append(cheb[:, n])
        columns += [cheb[:, n - a] + cheb[:, n + a] for a in range(1, LOW + 1)]
        columns += [cheb[:, n - a] - cheb[:, n + a] for a in range(1, LOW + 1)]
    matrix = np.stack(columns, axis=1)
    assert matrix.shape == (L, TOP + 1)
    return np.repeat(matrix, 8, axis=1).astype(np.float32)


BASIS = basis_matrix()


def basis_functions(x):
    y = x + x
    t, u = [jnp.ones_like(x), x], [jnp.ones_like(x), y]
    for k in range(2, LOW + 1):
        t.append(y * t[k - 1] - t[k - 2])
        if k < LOW:
            u.append(y * u[k - 1] - u[k - 2])
    square = 1.0 - x * x
    double = t[9] + t[9]
    t18, u17 = double * t[9] - 1.0, double * u[8]
    v18 = square * u17
    double = t18 + t18
    t36, v36 = double * t18 - 1.0, double * v18
    t37, v37 = t36 * x - v36, v36 * x + t36 * square
    t19, u18 = t18 * x - v18, u17 * x + t18
    v19 = square * u18
    t56, v56 = t37 * t19 - v37 * u18, v37 * t19 + t37 * v19
    low_t = [None] + [value.astype(bf16) for value in t[1:]]
    low_u = [None] + [value.astype(bf16) for value in u[1:]]
    yield from low_t[1:LOW]
    for tn, vn in ((t18, v18), (t37, v37), (t56, v56)):
        tn, vn = tn.astype(bf16), vn.astype(bf16)
        yield tn
        for a in range(1, LOW + 1):
            yield tn * low_t[a]
        yield vn
        for a in range(2, LOW + 1):
            yield vn * low_u[a - 1]


def partial_kernel(place_ref, cov_ref, maps_ref, out_ref):
    r = place_ref[0]
    product = lax.dot_general(
        cov_ref[...], maps_ref[...], (((1,), (1,)), ((), ())), preferred_element_type=f32
    )
    for g in range(NR):
        flip = (r >= g).astype(jnp.int32)
        for s in range(2):
            piece = NR * s + g
            rows = product[PIECE * piece : PIECE * (piece + 1)]
            out_ref[2 * g + jnp.where(flip == 1, 1 - s, s)] = rows


def spectra_kernel(
    place_ref, cos_ref, rows_ref, cols_ref, basis_ref, out_ref, maps, weights, even, odd, total
):
    r, c = place_ref[0], place_ref[1]
    group, own = c // 2, c % 2
    other = 1 - own
    diagonal = group == r
    half = jnp.where(group > r, own, other)
    zeros = jnp.zeros((PIECE, LANES - MAPS), bf16)
    row_sum = col_sum = jnp.zeros((8, LANES), f32)
    for place in range(NR):
        rows = jnp.concatenate([rows_ref[place], zeros], axis=1)
        at = pl.multiple_of((group ^ ORDER[place]) * PIECE, PIECE)
        maps[pl.ds(at, PIECE)] = rows
        cols = jnp.concatenate([cols_ref[place], zeros], axis=1)
        at = pl.multiple_of((r ^ ORDER[place]) * PIECE, PIECE)
        weights[pl.ds(at, PIECE)] = cols
        maps[pl.ds(CHUNK + at, PIECE)] = cols
        row_sum += jnp.sum(rows.astype(f32).reshape(PIECE // 8, 8, LANES), axis=0)
        col_sum += jnp.sum(cols.astype(f32).reshape(PIECE // 8, 8, LANES), axis=0)
    row_sum = jnp.sum(row_sum, axis=0, keepdims=True)
    col_sum = jnp.sum(col_sum, axis=0, keepdims=True)
    alpha = jnp.where(diagonal, 0.5, 1.0)
    beta = jnp.where(diagonal, 0.5, 0.0)
    total[...] = jnp.zeros_like(total)
    total[0, 0:1] = col_sum * (alpha * row_sum + beta * col_sum)

    def tile(t):
        part, first = t // 8, 32 * (t % 8)
        plain_row = 32 * (t % 16)
        plain = (CHUNK * half + plain_row, plain_row, t // 16, 1.0)
        mine = part < 3
        low = jnp.logical_or(part == 2, jnp.logical_and(part == 4, own == 1))
        row = first + jnp.where(low, 256, 0)
        column = jnp.where(mine, jnp.minimum(part, 1), jnp.where(part == 3, own, 1))
        weight = jnp.where(jnp.logical_or(part == 0, part == 2), 0.5, 1.0)
        chosen = (
            CHUNK * jnp.where(mine, own, other) + row,
            CHUNK * jnp.where(mine, 1, 0) + row,
            column,
            weight,
        )
        return [jnp.where(diagonal, a, b) for a, b in zip(chosen, plain)]

    def generate(t, slot):
        cos_row, _, column, _ = tile(t)
        cos_row = pl.multiple_of(cos_row, ROWS)
        column = pl.multiple_of(column * COLS, COLS)
        for first in range(0, ROWS, 16):
            x = cos_ref[pl.ds(cos_row + first, 16), pl.ds(column, COLS)]
            for k, value in enumerate(basis_functions(x)):
                slot[k, first : first + 16] = value

    def contract(t, slot):
        _, map_row, column, weight = tile(t)
        left = maps[pl.ds(pl.multiple_of(map_row, ROWS), ROWS)].astype(f32) * weight
        right = weights[pl.ds(pl.multiple_of(column * COLS, COLS), COLS)]
        image = jnp.dot(slot[...].reshape(TOP * ROWS, COLS), right, preferred_element_type=f32)
        for k in range(TOP):
            product = image[ROWS * k : ROWS * (k + 1)] * left
            total[k + 1] += jnp.sum(product.reshape(ROWS // 8, 8, LANES), axis=0)

    count = jnp.where(diagonal, 40, 32)
    generate(0, even)

    def step(pair, carry):
        t = 2 * pair
        generate(t + 1, odd)
        contract(t, even)
        generate(jnp.minimum(t + 2, count - 1), even)
        contract(t + 1, odd)
        return carry

    lax.fori_loop(0, count // 2, step, 0)
    sums = total[...].reshape((TOP + 1) * 8, LANES)
    spectra = jnp.dot(
        basis_ref[...], sums, preferred_element_type=f32, precision=lax.Precision.HIGHEST
    )
    out_ref[...] = spectra[:, :MAPS]


def assemble_kernel(place_ref, rows_ref, other_ref, out_ref, scratch):
    r, c = place_ref[0], place_ref[1]
    group = c // 2
    half = jnp.where(group > r, c % 2, 1 - c % 2)
    for place in range(NR):
        at = (group ^ ORDER[place]) * PIECE
        scratch[pl.ds(pl.multiple_of(CHUNK * half + at, PIECE), PIECE)] = rows_ref[place]
        scratch[pl.ds(pl.multiple_of(CHUNK * (1 - half) + at, PIECE), PIECE)] = other_ref[place]
    out_ref[...] = scratch[...].T


SMEM = pl.BlockSpec(memory_space=pltpu.SMEM)
VMEM = pl.BlockSpec(memory_space=pltpu.VMEM)


def partial_products(place, cov, maps):
    return pl.pallas_call(
        partial_kernel,
        out_shape=jax.ShapeDtypeStruct((NC, PIECE, MAPS), f32),
        in_specs=[SMEM, VMEM, VMEM],
        out_specs=VMEM,
        name="partial",
    )(place, cov, maps)


def block_spectra(place, cosines, rows, cols):
    return pl.pallas_call(
        spectra_kernel,
        out_shape=jax.ShapeDtypeStruct((L, MAPS), f32),
        in_specs=[SMEM, VMEM, VMEM, VMEM, VMEM],
        out_specs=VMEM,
        scratch_shapes=[
            pltpu.VMEM((2 * CHUNK, LANES), bf16),
            pltpu.VMEM((CHUNK, LANES), bf16),
            pltpu.VMEM((TOP, ROWS, COLS), bf16),
            pltpu.VMEM((TOP, ROWS, COLS), bf16),
            pltpu.VMEM((TOP + 1, 8, LANES), f32),
        ],
        cost_estimate=pl.CostEstimate(flops=9 * 10**9, bytes_accessed=4 * 10**6, transcendentals=0),
        name="spectra",
    )(place, cosines, rows, cols, jnp.asarray(BASIS))


def assemble(place, rows, other):
    return pl.pallas_call(
        assemble_kernel,
        out_shape=jax.ShapeDtypeStruct((MAPS, 2 * CHUNK), bf16),
        in_specs=[SMEM, VMEM, VMEM],
        out_specs=VMEM,
        scratch_shapes=[pltpu.VMEM((2 * CHUNK, MAPS), bf16)],
        name="assemble",
    )(place, rows, other).T


def everywhere(value):
    value = value + lax.ppermute(value, PROW[1], [(0, 1), (1, 0)])
    for axis in (PROW[0],) + PCOL:
        value = value + lax.ppermute(value, axis, [(0, 1), (1, 0), (2, 3), (3, 2)])
        value = value + lax.ppermute(value, axis, [(0, 3), (3, 0), (2, 1), (1, 2)])
    return value


def per_device(inverse_cov, cosines, sky_maps):
    place = jnp.stack([lax.axis_index(PROW), lax.axis_index(PCOL)]).astype(jnp.int32)
    partial = partial_products(place, inverse_cov, sky_maps.T)
    parts = lax.all_to_all(partial.astype(f16), PCOL, 0, 0, tiled=True)
    piece = jnp.sum(parts.astype(f32), axis=0).astype(bf16)

    cols = lax.ppermute(piece, ALL, TO_COLUMNS)[None]
    rows = piece[None]
    for row_step, column_step in zip(ROW_STEPS, COLUMN_STEPS):
        rows = jnp.concatenate([rows, lax.ppermute(rows, ALL, row_step)])
        cols = jnp.concatenate([cols, lax.ppermute(cols, ALL, column_step)])
    other = lax.ppermute(rows, ALL, OTHER_HALF)

    spectra = everywhere(block_spectra(place, cosines, rows, cols))
    return assemble(place, rows, other), spectra


def solution(mesh):
    split = Mesh(mesh.devices.reshape(4, 2, 4, 4), ALL)
    placed = (P(PROW, PCOL), P(PROW, PCOL), P(PCOL, None))
    return jax.shard_map(
        per_device, mesh=split, in_specs=placed, out_specs=(P(PROW, None), P()), check_vma=False
    )
```

```python
import functools

import jax
import jax.numpy as jnp
import numpy as np
from jax import lax
from jax.experimental import pallas as pl
from jax.experimental.pallas import tpu as pltpu
from jax.sharding import Mesh
from jax.sharding import PartitionSpec as P

NPIX = 8192
MAPS = 192
L = 64
LMIN = 2
TOP = LMIN + L - 1
NR, NC = 8, 16
CHUNK = NPIX // NC
PIECE = CHUNK // NR
LANES = 256
ROWS = 32
COLS = 256
LOW = 9
CENTRES = (18, 37, 56)
CENTRE = 2 * LOW - 1
FACTORS = CENTRE + 2 * len(CENTRES)
LAG = 28
PROW = ("prow_0", "prow_1")
PCOL = ("pcol_0", "pcol_1")
ALL = PROW + PCOL
bf16, f16, f32 = jnp.bfloat16, jnp.float16, jnp.float32
MASKS = (1, 2, 6)
ORDER = (0, 1, 2, 3, 6, 7, 4, 5)


def half_of(r, c):
    return c % 2 if c // 2 > r else 1 - c % 2


MEMBERS = [
    [[c for c in range(NC) if half_of(r, c) == s] for s in range(2)] for r in range(NR)
]
EACH = [(r, s, g) for r in range(NR) for s in range(2) for g in range(NR)]
TO_COLUMNS = [(r * NC + MEMBERS[r][s][g], g * NC + 2 * r + s) for r, s, g in EACH]
OTHER_HALF = [(r * NC + MEMBERS[r][s][g], r * NC + MEMBERS[r][1 - s][g]) for r, s, g in EACH]
ROW_STEPS = [
    [(r * NC + MEMBERS[r][s][g], r * NC + MEMBERS[r][s][g ^ mask]) for r, s, g in EACH]
    for mask in MASKS
]
COLUMN_STEPS = [
    [(r * NC + c, (r ^ mask) * NC + c) for r in range(NR) for c in range(NC)] for mask in MASKS
]


def basis_matrix():
    g = [1.0]
    for k in range(1, TOP + 1):
        g.append(g[-1] * (2 * k - 1) / (2 * k))
    cheb = np.zeros((L, TOP + 1))
    for row in range(L):
        degree = row + LMIN
        for k in range(degree + 1):
            cheb[row, abs(degree - 2 * k)] += g[k] * g[degree - k]
        cheb[row] *= 2.0 * (2.0 * degree + 1.0) / NPIX
    columns = [cheb[:, k] for k in range(LOW)]
    for n in CENTRES:
        columns.append(cheb[:, n])
        columns += [cheb[:, n - a] + cheb[:, n + a] for a in range(1, LOW + 1)]
        columns += [cheb[:, n - a] - cheb[:, n + a] for a in range(1, LOW + 1)]
    matrix = np.stack(columns, axis=1)
    assert matrix.shape == (L, TOP + 1)
    return matrix.astype(np.float32)


BASIS = basis_matrix()


def factors(x):
    y = x + x
    t, u = [jnp.ones_like(x), x], [jnp.ones_like(x), y]
    yield 0, x.astype(bf16)
    yield LOW, y.astype(bf16)
    for k in range(2, LOW + 1):
        t.append(y * t[k - 1] - t[k - 2])
        yield k - 1, t[k].astype(bf16)
        if k < LOW:
            u.append(y * u[k - 1] - u[k - 2])
            yield LOW + k - 1, u[k].astype(bf16)
    t9, u8 = t[9], u[8]
    square = 1.0 - x * x
    double = t9 + t9
    t18, u17 = double * t9 - 1.0, double * u8
    v18 = square * u17
    yield CENTRE, t18.astype(bf16)
    yield CENTRE + 1, v18.astype(bf16)
    double = t18 + t18
    t36, v36 = double * t18 - 1.0, double * v18
    t37, v37 = t36 * x - v36, v36 * x + t36 * square
    yield CENTRE + 2, t37.astype(bf16)
    yield CENTRE + 3, v37.astype(bf16)
    t19, u18 = t18 * x - v18, u17 * x + t18
    v19 = square * u18
    t56, v56 = t37 * t19 - v37 * u18, v37 * t19 + t37 * v19
    yield CENTRE + 4, t56.astype(bf16)
    yield CENTRE + 5, v56.astype(bf16)


def basis_function(k, made):
    if k < LOW - 1:
        return made[k]
    centre, which = divmod(k - (LOW - 1), 2 * LOW + 1)
    tn, vn = CENTRE + 2 * centre, CENTRE + 2 * centre + 1
    if which == 0:
        return made[tn]
    if which <= LOW:
        return made[tn] * made[which - 1]
    if which == LOW + 1:
        return made[vn]
    return made[vn] * made[LOW + which - LOW - 2]


def partial_kernel(place_ref, cov_ref, maps_ref, out_ref):
    r = place_ref[0]
    product = lax.dot_general(
        cov_ref[...], maps_ref[...], (((1,), (1,)), ((), ())), preferred_element_type=f32
    )
    for g in range(NR):
        flip = (r >= g).astype(jnp.int32)
        for s in range(2):
            piece = NR * s + g
            rows = product[PIECE * piece : PIECE * (piece + 1)]
            out_ref[2 * g + jnp.where(flip == 1, 1 - s, s)] = rows


def spectra_kernel(
    place_ref, cos_ref, r0, r1, r2, r3, c0, c1, c2, c3, basis_ref, out_ref,
    maps, weights, even, odd, total,
):
    def with_sums(*sums):
        spectra_body(
            place_ref, cos_ref, (r0, r1, r2, r3), (c0, c1, c2, c3), basis_ref, out_ref,
            maps, weights, even, odd, total, (sums[:17], sums[17:]),
        )

    pl.run_scoped(
        with_sums,
        *[pltpu.ACC(0)((ROWS, LANES), f32)] * 17,
        *[pltpu.ACC(1)((ROWS, LANES), f32)] * 16,
    )


def pieces_of(refs):
    return [(ref, at) for ref in refs for at in range(ref.shape[0])]


def spectra_body(
    place_ref, cos_ref, rows_refs, cols_refs, basis_ref, out_ref,
    maps, weights, even, odd, total, sums,
):
    r, c = place_ref[0], place_ref[1]
    group, own = c // 2, c % 2
    other = 1 - own
    diagonal = group == r
    half = jnp.where(group > r, own, other)
    zeros = jnp.zeros((PIECE, LANES - MAPS), bf16)
    row_sum = col_sum = jnp.zeros((8, LANES), f32)
    for order, (rows_ref, at), (cols_ref, _) in zip(ORDER, pieces_of(rows_refs), pieces_of(cols_refs)):
        rows = jnp.concatenate([rows_ref[at], zeros], axis=1)
        maps[pl.ds(pl.multiple_of((group ^ order) * PIECE, PIECE), PIECE)] = rows
        cols = jnp.concatenate([cols_ref[at], zeros], axis=1)
        to = pl.multiple_of((r ^ order) * PIECE, PIECE)
        weights[pl.ds(to, PIECE)] = cols
        maps[pl.ds(CHUNK + to, PIECE)] = cols
        row_sum += jnp.sum(rows.astype(f32).reshape(PIECE // 8, 8, LANES), axis=0)
        col_sum += jnp.sum(cols.astype(f32).reshape(PIECE // 8, 8, LANES), axis=0)
    row_sum = jnp.sum(row_sum, axis=0, keepdims=True)
    col_sum = jnp.sum(col_sum, axis=0, keepdims=True)
    alpha = jnp.where(diagonal, 0.5, 1.0)
    beta = jnp.where(diagonal, 0.5, 0.0)
    total[...] = jnp.zeros_like(total)
    total[0, 0:1] = col_sum * (alpha * row_sum + beta * col_sum)
    count = jnp.where(diagonal, 40, 32)

    def tile(t):
        part, first = t // 8, 32 * (t % 8)
        plain_row = 32 * (t % 16)
        plain = (CHUNK * half + plain_row, plain_row, t // 16, 1.0)
        mine = part < 3
        low = jnp.logical_or(part == 2, jnp.logical_and(part == 4, own == 1))
        row = first + jnp.where(low, 256, 0)
        column = jnp.where(mine, jnp.minimum(part, 1), jnp.where(part == 3, own, 1))
        weight = jnp.where(jnp.logical_or(part == 0, part == 2), 0.5, 1.0)
        chosen = (
            CHUNK * jnp.where(mine, own, other) + row,
            CHUNK * jnp.where(mine, 1, 0) + row,
            column,
            weight,
        )
        return [jnp.where(diagonal, a, b) for a, b in zip(chosen, plain)]

    def generate(t, slot):
        cos_row, _, column, _ = tile(t)
        cos_row = pl.multiple_of(cos_row, ROWS)
        column = pl.multiple_of(column * COLS, COLS)
        for first in range(0, ROWS, 16):
            x = cos_ref[pl.ds(cos_row + first, 16), pl.ds(column, COLS)]
            for which, value in factors(x):
                slot[which, first : first + 16] = value
                yield

    def stage(t):
        column = tile(t)[2]
        right = weights[pl.ds(pl.multiple_of(column * COLS, COLS), COLS)]
        for unit in range(2):
            pltpu.matmul_push_rhs(right, 0, unit)

    def left_of(t):
        _, map_row, _, weight = tile(t)
        return maps[pl.ds(pl.multiple_of(map_row, ROWS), ROWS)].astype(f32) * weight

    def sum_of(k):
        unit, turn = k % 2, k // 2
        return sums[unit][turn % 16 if turn < 32 else 16]

    def take(k, left):
        product = pltpu.matmul_pop(sum_of(k)) * left
        total[k + 1] += jnp.sum(product.reshape(ROWS // 8, 8, LANES), axis=0)

    def process(t, now, later):
        following = jnp.minimum(t + 1, count - 1)
        making = generate(following, later)
        left = left_of(jnp.maximum(t - 1, 0))
        for k in range(TOP):
            take((k - LAG) % TOP, left)
            if k == LAG - 1:
                left = left_of(t)
            pltpu.matmul_acc_lhs(
                sum_of(k), basis_function(k, now), load_staged_rhs=0 if k < 2 else None
            )
            if k == 8:
                stage(following)
            next(making, None)
        for _ in making:
            pass

    for one in sums[0] + sums[1]:
        pltpu.matmul_pop(one)
    for _ in generate(0, even):
        pass
    stage(0)

    def step(pair, carry):
        process(2 * pair, even, odd)
        process(2 * pair + 1, odd, even)
        return carry

    lax.fori_loop(0, count // 2, step, 0)
    left = left_of(count - 1)
    for k in range(TOP - LAG, TOP):
        take(k, left)
    for unit in range(2):
        pltpu.matmul_acc_lhs(sums[unit][0], jnp.zeros((ROWS, COLS), bf16), load_staged_rhs=0)
        pltpu.matmul_pop(sums[unit][0])

    spectra = jnp.zeros((L, LANES), f32)
    for k in range(TOP + 1):
        spectra += basis_ref[:, k : k + 1] * jnp.sum(total[k], axis=0, keepdims=True)
    out_ref[...] = spectra[:, :MAPS]


def assemble_kernel(place_ref, r0, r1, r2, r3, other_ref, out_ref, scratch):
    r, c = place_ref[0], place_ref[1]
    group = c // 2
    half = jnp.where(group > r, c % 2, 1 - c % 2)
    for place, (ref, one) in enumerate(pieces_of((r0, r1, r2, r3))):
        at = (group ^ ORDER[place]) * PIECE
        scratch[pl.ds(pl.multiple_of(CHUNK * half + at, PIECE), PIECE)] = ref[one]
        scratch[pl.ds(pl.multiple_of(CHUNK * (1 - half) + at, PIECE), PIECE)] = other_ref[place]
    out_ref[...] = scratch[...].T


SMEM = pl.BlockSpec(memory_space=pltpu.SMEM)
VMEM = pl.BlockSpec(memory_space=pltpu.VMEM)


def partial_products(place, cov, maps):
    return pl.pallas_call(
        partial_kernel,
        out_shape=jax.ShapeDtypeStruct((NC, PIECE, MAPS), f32),
        in_specs=[SMEM, VMEM, VMEM],
        out_specs=VMEM,
        name="partial",
    )(place, cov, maps)


def block_spectra(place, cosines, rows, cols):
    return pl.pallas_call(
        spectra_kernel,
        out_shape=jax.ShapeDtypeStruct((L, MAPS), f32),
        in_specs=[SMEM] + [VMEM] * 10,
        out_specs=VMEM,
        scratch_shapes=[
            pltpu.VMEM((2 * CHUNK, LANES), bf16),
            pltpu.VMEM((CHUNK, LANES), bf16),
            pltpu.VMEM((FACTORS, ROWS, COLS), bf16),
            pltpu.VMEM((FACTORS, ROWS, COLS), bf16),
            pltpu.VMEM((TOP + 1, 8, LANES), f32),
        ],
        cost_estimate=pl.CostEstimate(flops=9 * 10**9, bytes_accessed=4 * 10**6, transcendentals=0),
        name="spectra",
    )(place, cosines, *rows, *cols, jnp.asarray(BASIS))


def assemble(place, rows, other):
    return pl.pallas_call(
        assemble_kernel,
        out_shape=jax.ShapeDtypeStruct((MAPS, 2 * CHUNK), bf16),
        in_specs=[SMEM] + [VMEM] * 5,
        out_specs=VMEM,
        scratch_shapes=[pltpu.VMEM((2 * CHUNK, MAPS), bf16)],
        name="assemble",
    )(place, *rows, other).T


def everywhere(value):
    value = value + lax.ppermute(value, PROW[1], [(0, 1), (1, 0)])
    for axis in (PROW[0],) + PCOL:
        value = value + lax.ppermute(value, axis, [(0, 1), (1, 0), (2, 3), (3, 2)])
        value = value + lax.ppermute(value, axis, [(0, 3), (3, 0), (2, 1), (1, 2)])
    return value


def per_device(inverse_cov, cosines, sky_maps):
    place = jnp.stack([lax.axis_index(PROW), lax.axis_index(PCOL)]).astype(jnp.int32)
    partial = partial_products(place, inverse_cov, sky_maps.T)
    parts = lax.all_to_all(partial.astype(f16), PCOL, 0, 0, tiled=True)
    piece = jnp.sum(parts.astype(f32), axis=0).astype(bf16)

    cols, rows = [lax.ppermute(piece, ALL, TO_COLUMNS)[None]], [piece[None]]
    for row_step, column_step in zip(ROW_STEPS, COLUMN_STEPS):
        rows.append(lax.ppermute(jnp.concatenate(rows), ALL, row_step))
        cols.append(lax.ppermute(jnp.concatenate(cols), ALL, column_step))
    other = lax.ppermute(jnp.concatenate(rows), ALL, OTHER_HALF)

    spectra = everywhere(block_spectra(place, cosines, rows, cols))
    return assemble(place, rows, other), spectra


def solution(mesh):
    split = Mesh(mesh.devices.reshape(4, 2, 4, 4), ALL)
    placed = (P(PROW, PCOL), P(PROW, PCOL), P(PCOL, None))
    return jax.shard_map(
        per_device, mesh=split, in_specs=placed, out_specs=(P(PROW, None), P()), check_vma=False
    )
```

```python
import functools

import jax
import jax.numpy as jnp
import numpy as np
from jax import lax
from jax.experimental import pallas as pl
from jax.experimental.pallas import tpu as pltpu
from jax.sharding import Mesh
from jax.sharding import PartitionSpec as P

NPIX = 8192
MAPS = 192
L = 64
LMIN = 2
TOP = LMIN + L - 1
NR, NC = 8, 16
CHUNK = NPIX // NC
PIECE = CHUNK // NR
LANES = 256
ROWS = 32
COLS = 256
LOW = 9
CENTRES = (18, 37, 56)
CENTRE = 2 * LOW - 1
FACTORS = CENTRE + 2 * len(CENTRES)
LAG = 28
PROW = ("prow_0", "prow_1")
PCOL = ("pcol_0", "pcol_1")
ALL = PROW + PCOL
bf16, f16, f32 = jnp.bfloat16, jnp.float16, jnp.float32
MASKS = (1, 2, 6)
ORDER = (0, 1, 2, 3, 6, 7, 4, 5)


def half_of(r, c):
    return c % 2 if c // 2 > r else 1 - c % 2


MEMBERS = [
    [[c for c in range(NC) if half_of(r, c) == s] for s in range(2)] for r in range(NR)
]
EACH = [(r, s, g) for r in range(NR) for s in range(2) for g in range(NR)]
TO_COLUMNS = [(r * NC + MEMBERS[r][s][g], g * NC + 2 * r + s) for r, s, g in EACH]
OTHER_HALF = [(r * NC + MEMBERS[r][s][g], r * NC + MEMBERS[r][1 - s][g]) for r, s, g in EACH]
SUMMERS = [[r * NC + MEMBERS[r][s][g] for s in range(2) for g in range(NR)] for r in range(NR)]
ROW_STEPS = [
    [(r * NC + MEMBERS[r][s][g], r * NC + MEMBERS[r][s][g ^ mask]) for r, s, g in EACH]
    for mask in MASKS
]
COLUMN_STEPS = [
    [(r * NC + c, (r ^ mask) * NC + c) for r in range(NR) for c in range(NC)] for mask in MASKS
]


def basis_matrix():
    g = [1.0]
    for k in range(1, TOP + 1):
        g.append(g[-1] * (2 * k - 1) / (2 * k))
    cheb = np.zeros((L, TOP + 1))
    for row in range(L):
        degree = row + LMIN
        for k in range(degree + 1):
            cheb[row, abs(degree - 2 * k)] += g[k] * g[degree - k]
        cheb[row] *= 2.0 * (2.0 * degree + 1.0) / NPIX
    columns = [cheb[:, k] for k in range(LOW)]
    for n in CENTRES:
        columns.append(cheb[:, n])
        columns += [cheb[:, n - a] + cheb[:, n + a] for a in range(1, LOW + 1)]
        columns += [cheb[:, n - a] - cheb[:, n + a] for a in range(1, LOW + 1)]
    matrix = np.stack(columns, axis=1)
    assert matrix.shape == (L, TOP + 1)
    return matrix.astype(np.float32)


BASIS = basis_matrix()


def factors(x):
    y = x + x
    t, u = [jnp.ones_like(x), x], [jnp.ones_like(x), y]
    yield 0, x.astype(bf16)
    yield LOW, y.astype(bf16)
    for k in range(2, LOW + 1):
        t.append(y * t[k - 1] - t[k - 2])
        yield k - 1, t[k].astype(bf16)
        if k < LOW:
            u.append(y * u[k - 1] - u[k - 2])
            yield LOW + k - 1, u[k].astype(bf16)
    t9, u8 = t[9], u[8]
    square = 1.0 - x * x
    double = t9 + t9
    t18, u17 = double * t9 - 1.0, double * u8
    v18 = square * u17
    yield CENTRE, t18.astype(bf16)
    yield CENTRE + 1, v18.astype(bf16)
    double = t18 + t18
    t36, v36 = double * t18 - 1.0, double * v18
    t37, v37 = t36 * x - v36, v36 * x + t36 * square
    yield CENTRE + 2, t37.astype(bf16)
    yield CENTRE + 3, v37.astype(bf16)
    t19, u18 = t18 * x - v18, u17 * x + t18
    v19 = square * u18
    t56, v56 = t37 * t19 - v37 * u18, v37 * t19 + t37 * v19
    yield CENTRE + 4, t56.astype(bf16)
    yield CENTRE + 5, v56.astype(bf16)


def basis_function(k, made):
    if k < LOW - 1:
        return made[k]
    centre, which = divmod(k - (LOW - 1), 2 * LOW + 1)
    tn, vn = CENTRE + 2 * centre, CENTRE + 2 * centre + 1
    if which == 0:
        return made[tn]
    if which <= LOW:
        return made[tn] * made[which - 1]
    if which == LOW + 1:
        return made[vn]
    return made[vn] * made[LOW + which - LOW - 2]


def spectra_kernel(
    place_ref, cos_ref, r0, r1, r2, r3, c0, c1, c2, c3, basis_ref, out_ref, half_ref,
    maps, weights, even, odd, total,
):
    def with_sums(*sums):
        spectra_body(
            place_ref, cos_ref, (r0, r1, r2, r3), (c0, c1, c2, c3), basis_ref, out_ref, half_ref,
            maps, weights, even, odd, total, (sums[:17], sums[17:]),
        )

    pl.run_scoped(
        with_sums,
        *[pltpu.ACC(0)((ROWS, LANES), f32)] * 17,
        *[pltpu.ACC(1)((ROWS, LANES), f32)] * 16,
    )


def pieces_of(refs):
    return [(ref, at) for ref in refs for at in range(ref.shape[0])]


def spectra_body(
    place_ref, cos_ref, rows_refs, cols_refs, basis_ref, out_ref, half_ref,
    maps, weights, even, odd, total, sums,
):
    r, c = place_ref[0], place_ref[1]
    group, own = c // 2, c % 2
    other = 1 - own
    diagonal = group == r
    half = jnp.where(group > r, own, other)
    zeros = jnp.zeros((PIECE, LANES - MAPS), bf16)
    row_sum = col_sum = jnp.zeros((8, LANES), f32)
    for order, (rows_ref, at), (cols_ref, _) in zip(ORDER, pieces_of(rows_refs), pieces_of(cols_refs)):
        rows = jnp.concatenate([rows_ref[at], zeros], axis=1)
        to = pl.multiple_of((group ^ order) * PIECE, PIECE)
        maps[pl.ds(to, PIECE)] = rows
        half_ref[pl.ds(to, PIECE)] = rows_ref[at]
        cols = jnp.concatenate([cols_ref[at], zeros], axis=1)
        to = pl.multiple_of((r ^ order) * PIECE, PIECE)
        weights[pl.ds(to, PIECE)] = cols
        maps[pl.ds(CHUNK + to, PIECE)] = cols
        row_sum += jnp.sum(rows.astype(f32).reshape(PIECE // 8, 8, LANES), axis=0)
        col_sum += jnp.sum(cols.astype(f32).reshape(PIECE // 8, 8, LANES), axis=0)
    row_sum = jnp.sum(row_sum, axis=0, keepdims=True)
    col_sum = jnp.sum(col_sum, axis=0, keepdims=True)
    alpha = jnp.where(diagonal, 0.5, 1.0)
    beta = jnp.where(diagonal, 0.5, 0.0)
    total[...] = jnp.zeros_like(total)
    total[0, 0:1] = col_sum * (alpha * row_sum + beta * col_sum)
    count = jnp.where(diagonal, 40, 32)

    def tile(t):
        part, first = t // 8, 32 * (t % 8)
        plain_row = 32 * (t % 16)
        plain = (CHUNK * half + plain_row, plain_row, t // 16, 1.0)
        mine = part < 3
        low = jnp.logical_or(part == 2, jnp.logical_and(part == 4, own == 1))
        row = first + jnp.where(low, 256, 0)
        column = jnp.where(mine, jnp.minimum(part, 1), jnp.where(part == 3, own, 1))
        weight = jnp.where(jnp.logical_or(part == 0, part == 2), 0.5, 1.0)
        chosen = (
            CHUNK * jnp.where(mine, own, other) + row,
            CHUNK * jnp.where(mine, 1, 0) + row,
            column,
            weight,
        )
        return [jnp.where(diagonal, a, b) for a, b in zip(chosen, plain)]

    def generate(t, slot):
        cos_row, _, column, _ = tile(t)
        cos_row = pl.multiple_of(cos_row, ROWS)
        column = pl.multiple_of(column * COLS, COLS)
        for first in range(0, ROWS, 16):
            x = cos_ref[pl.ds(cos_row + first, 16), pl.ds(column, COLS)]
            for which, value in factors(x):
                slot[which, first : first + 16] = value
                yield

    def stage(t):
        column = tile(t)[2]
        right = weights[pl.ds(pl.multiple_of(column * COLS, COLS), COLS)]
        for unit in range(2):
            pltpu.matmul_push_rhs(right, 0, unit)

    def left_of(t):
        _, map_row, _, weight = tile(t)
        return maps[pl.ds(pl.multiple_of(map_row, ROWS), ROWS)].astype(f32) * weight

    def sum_of(k):
        unit, turn = k % 2, k // 2
        return sums[unit][turn % 16 if turn < 32 else 16]

    def take(k, left):
        product = pltpu.matmul_pop(sum_of(k)) * left
        total[k + 1] += jnp.sum(product.reshape(ROWS // 8, 8, LANES), axis=0)

    def process(t, now, later):
        following = jnp.minimum(t + 1, count - 1)
        making = generate(following, later)
        left = left_of(jnp.maximum(t - 1, 0))
        for k in range(TOP):
            take((k - LAG) % TOP, left)
            if k == LAG - 1:
                left = left_of(t)
            pltpu.matmul_acc_lhs(
                sum_of(k), basis_function(k, now), load_staged_rhs=0 if k < 2 else None
            )
            if k == 8:
                stage(following)
            next(making, None)
        for _ in making:
            pass

    for one in sums[0] + sums[1]:
        pltpu.matmul_pop(one)
    for _ in generate(0, even):
        pass
    stage(0)

    def step(pair, carry):
        process(2 * pair, even, odd)
        process(2 * pair + 1, odd, even)
        return carry

    lax.fori_loop(0, count // 2, step, 0)
    left = left_of(count - 1)
    for k in range(TOP - LAG, TOP):
        take(k, left)
    for unit in range(2):
        pltpu.matmul_acc_lhs(sums[unit][0], jnp.zeros((ROWS, COLS), bf16), load_staged_rhs=0)
        pltpu.matmul_pop(sums[unit][0])

    spectra = jnp.zeros((L, LANES), f32)
    for k in range(TOP + 1):
        spectra += basis_ref[:, k : k + 1] * jnp.sum(total[k], axis=0, keepdims=True)
    out_ref[...] = spectra[:, :MAPS]


def assemble_kernel(place_ref, half_ref, other_ref, out_ref, scratch):
    r, c = place_ref[0], place_ref[1]
    half = jnp.where(c // 2 > r, c % 2, 1 - c % 2)
    scratch[pl.ds(pl.multiple_of(CHUNK * half, CHUNK), CHUNK)] = half_ref[...]
    scratch[pl.ds(pl.multiple_of(CHUNK * (1 - half), CHUNK), CHUNK)] = other_ref[...]
    out_ref[...] = scratch[...].T


SMEM = pl.BlockSpec(memory_space=pltpu.SMEM)
VMEM = pl.BlockSpec(memory_space=pltpu.VMEM)


def block_spectra(place, cosines, rows, cols):
    return pl.pallas_call(
        spectra_kernel,
        out_shape=(pltpu.VMEM((L, MAPS), f32), pltpu.VMEM((CHUNK, MAPS), bf16)),
        in_specs=[SMEM] + [VMEM] * 10,
        out_specs=(VMEM, VMEM),
        scratch_shapes=[
            pltpu.VMEM((2 * CHUNK, LANES), bf16),
            pltpu.VMEM((CHUNK, LANES), bf16),
            pltpu.VMEM((FACTORS, ROWS, COLS), bf16),
            pltpu.VMEM((FACTORS, ROWS, COLS), bf16),
            pltpu.VMEM((TOP + 1, 8, LANES), f32),
        ],
        cost_estimate=pl.CostEstimate(flops=9 * 10**9, bytes_accessed=4 * 10**6, transcendentals=0),
        compiler_params=pltpu.CompilerParams(
            vmem_limit_bytes=24 * 2**20,
        ),
        name="spectra",
    )(place, cosines, *rows, *cols, jnp.asarray(BASIS))


def assemble(place, half, other):
    return pl.pallas_call(
        assemble_kernel,
        out_shape=jax.ShapeDtypeStruct((MAPS, 2 * CHUNK), bf16),
        in_specs=[SMEM, VMEM, VMEM],
        out_specs=VMEM,
        scratch_shapes=[pltpu.VMEM((2 * CHUNK, MAPS), bf16)],
        compiler_params=pltpu.CompilerParams(vmem_limit_bytes=8 * 2**20),
        name="assemble",
    )(place, half, other).T


def everywhere(value):
    value = value + lax.ppermute(value, PROW[1], [(0, 1), (1, 0)])
    for axis in (PROW[0],) + PCOL:
        value = value + lax.ppermute(value, axis, [(0, 1), (1, 0), (2, 3), (3, 2)])
        value = value + lax.ppermute(value, axis, [(0, 3), (3, 0), (2, 1), (1, 2)])
    return value


def per_device(inverse_cov, cosines, sky_maps):
    place = jnp.stack([lax.axis_index(PROW), lax.axis_index(PCOL)]).astype(jnp.int32)
    partial = jnp.dot(inverse_cov, sky_maps, preferred_element_type=f32)
    partial = partial.astype(f16).reshape(NC, PIECE, MAPS)
    parts = lax.all_to_all(partial, ALL, 0, 0, axis_index_groups=SUMMERS, tiled=True)
    piece = jnp.sum(parts.astype(f32), axis=0).astype(bf16)

    cols, rows = [lax.ppermute(piece, ALL, TO_COLUMNS)[None]], [piece[None]]
    for row_step, column_step in zip(ROW_STEPS, COLUMN_STEPS):
        rows.append(lax.ppermute(jnp.concatenate(rows), ALL, row_step))
        cols.append(lax.ppermute(jnp.concatenate(cols), ALL, column_step))

    cosines = pltpu.with_memory_space_constraint(cosines, pltpu.VMEM)
    share, half = block_spectra(place, cosines, rows, cols)
    other = lax.ppermute(half, ALL, OTHER_HALF)
    spectra = everywhere(share)
    return assemble(place, half, other), spectra


def solution(mesh):
    split = Mesh(mesh.devices.reshape(4, 2, 4, 4), ALL)
    placed = (P(PROW, PCOL), P(PROW, PCOL), P(PCOL, None))
    return jax.shard_map(
        per_device, mesh=split, in_specs=placed, out_specs=(P(PROW, None), P()), check_vma=False
    )
```

```python
import functools

import jax
import jax.numpy as jnp
import numpy as np
from jax import lax
from jax.experimental import pallas as pl
from jax.experimental.layout import Layout, with_layout_constraint
from jax.experimental.pallas import tpu as pltpu
from jax.sharding import Mesh
from jax.sharding import PartitionSpec as P

NPIX = 8192
MAPS = 192
L = 64
LMIN = 2
TOP = LMIN + L - 1
NR, NC = 8, 16
CHUNK = NPIX // NC
PIECE = CHUNK // NR
LANES = 256
ROWS = 32
COLS = 256
LOW = 9
CENTRES = (18, 37, 56)
CENTRE = 2 * LOW - 1
FACTORS = CENTRE + 2 * len(CENTRES)
LAG = 28
PROW = ("prow_0", "prow_1")
PCOL = ("pcol_0", "pcol_1")
ALL = PROW + PCOL
bf16, f16, f32 = jnp.bfloat16, jnp.float16, jnp.float32
MASKS = (1, 2, 6, 4)
ORDER = (0, 1, 2, 3, 6, 7, 4, 5)


def half_of(r, c):
    return c % 2 if c // 2 > r else 1 - c % 2


MEMBERS = [
    [[c for c in range(NC) if half_of(r, c) == s] for s in range(2)] for r in range(NR)
]
EACH = [(r, s, g) for r in range(NR) for s in range(2) for g in range(NR)]
TO_COLUMNS = [(r * NC + MEMBERS[r][s][g], g * NC + 2 * r + s) for r, s, g in EACH]
OTHER_HALF = [(r * NC + MEMBERS[r][s][g], r * NC + MEMBERS[r][1 - s][g]) for r, s, g in EACH]
SUMMERS = [[r * NC + MEMBERS[r][s][g] for s in range(2) for g in range(NR)] for r in range(NR)]
ROW_STEPS = [
    [(r * NC + MEMBERS[r][s][g], r * NC + MEMBERS[r][s][g ^ mask]) for r, s, g in EACH]
    for mask in MASKS
]
COLUMN_STEPS = [
    [(r * NC + c, (r ^ mask) * NC + c) for r in range(NR) for c in range(NC)] for mask in MASKS
]


def basis_matrix():
    g = [1.0]
    for k in range(1, TOP + 1):
        g.append(g[-1] * (2 * k - 1) / (2 * k))
    cheb = np.zeros((L, TOP + 1))
    for row in range(L):
        degree = row + LMIN
        for k in range(degree + 1):
            cheb[row, abs(degree - 2 * k)] += g[k] * g[degree - k]
        cheb[row] *= 2.0 * (2.0 * degree + 1.0) / NPIX
    columns = [cheb[:, k] for k in range(LOW)]
    for n in CENTRES:
        columns.append(cheb[:, n])
        columns += [cheb[:, n - a] + cheb[:, n + a] for a in range(1, LOW + 1)]
        columns += [cheb[:, n - a] - cheb[:, n + a] for a in range(1, LOW + 1)]
    matrix = np.stack(columns, axis=1)
    assert matrix.shape == (L, TOP + 1)
    return matrix.astype(np.float32)


BASIS = basis_matrix()


def factors(x):
    y = x + x
    t, u = [jnp.ones_like(x), x], [jnp.ones_like(x), y]
    yield 0, x.astype(bf16)
    yield LOW, y.astype(bf16)
    for k in range(2, LOW + 1):
        t.append(y * t[k - 1] - t[k - 2])
        yield k - 1, t[k].astype(bf16)
        if k < LOW:
            u.append(y * u[k - 1] - u[k - 2])
            yield LOW + k - 1, u[k].astype(bf16)
    t9, u8 = t[9], u[8]
    square = 1.0 - x * x
    double = t9 + t9
    t18, u17 = double * t9 - 1.0, double * u8
    v18 = square * u17
    yield CENTRE, t18.astype(bf16)
    yield CENTRE + 1, v18.astype(bf16)
    double = t18 + t18
    t36, v36 = double * t18 - 1.0, double * v18
    t37, v37 = t36 * x - v36, v36 * x + t36 * square
    yield CENTRE + 2, t37.astype(bf16)
    yield CENTRE + 3, v37.astype(bf16)
    t19, u18 = t18 * x - v18, u17 * x + t18
    v19 = square * u18
    t56, v56 = t37 * t19 - v37 * u18, v37 * t19 + t37 * v19
    yield CENTRE + 4, t56.astype(bf16)
    yield CENTRE + 5, v56.astype(bf16)


def basis_function(k, made):
    if k < LOW - 1:
        return made[k]
    centre, which = divmod(k - (LOW - 1), 2 * LOW + 1)
    tn, vn = CENTRE + 2 * centre, CENTRE + 2 * centre + 1
    if which == 0:
        return made[tn]
    if which <= LOW:
        return made[tn] * made[which - 1]
    if which == LOW + 1:
        return made[vn]
    return made[vn] * made[LOW + which - LOW - 2]


def spectra_kernel(
    place_ref, cos_ref, r0, r1, r2, r3, c0, c1, c2, c3, basis_ref, out_ref, half_ref,
    maps, weights, even, odd, total,
):
    def with_sums(*sums):
        spectra_body(
            place_ref, cos_ref, (r0, r1, r2, r3), (c0, c1, c2, c3), basis_ref, out_ref, half_ref,
            maps, weights, even, odd, total, (sums[:17], sums[17:]),
        )

    pl.run_scoped(
        with_sums,
        *[pltpu.ACC(0)((ROWS, LANES), f32)] * 17,
        *[pltpu.ACC(1)((ROWS, LANES), f32)] * 16,
    )


def pieces_of(refs):
    return [(ref, at) for ref in refs for at in range(ref.shape[0])]


def spectra_body(
    place_ref, cos_ref, rows_refs, cols_refs, basis_ref, out_ref, half_ref,
    maps, weights, even, odd, total, sums,
):
    r, c = place_ref[0], place_ref[1]
    group, own = c // 2, c % 2
    other = 1 - own
    diagonal = group == r
    half = jnp.where(group > r, own, other)
    zeros = jnp.zeros((PIECE, LANES - MAPS), bf16)
    row_sum = col_sum = jnp.zeros((8, LANES), f32)
    for order, (rows_ref, at), (cols_ref, _) in zip(ORDER, pieces_of(rows_refs), pieces_of(cols_refs)):
        rows = jnp.concatenate([rows_ref[at], zeros], axis=1)
        to = pl.multiple_of((group ^ order) * PIECE, PIECE)
        maps[pl.ds(to, PIECE)] = rows
        half_ref[pl.ds(to, PIECE)] = rows_ref[at]
        cols = jnp.concatenate([cols_ref[at], zeros], axis=1)
        to = pl.multiple_of((r ^ order) * PIECE, PIECE)
        weights[pl.ds(to, PIECE)] = cols
        maps[pl.ds(CHUNK + to, PIECE)] = cols
        row_sum += jnp.sum(rows.astype(f32).reshape(PIECE // 8, 8, LANES), axis=0)
        col_sum += jnp.sum(cols.astype(f32).reshape(PIECE // 8, 8, LANES), axis=0)
    row_sum = jnp.sum(row_sum, axis=0, keepdims=True)
    col_sum = jnp.sum(col_sum, axis=0, keepdims=True)
    alpha = jnp.where(diagonal, 0.5, 1.0)
    beta = jnp.where(diagonal, 0.5, 0.0)
    total[...] = jnp.zeros_like(total)
    total[0, 0:1] = col_sum * (alpha * row_sum + beta * col_sum)
    count = jnp.where(diagonal, 40, 32)

    def tile(t):
        part, first = t // 8, 32 * (t % 8)
        plain_row = 32 * (t % 16)
        plain = (CHUNK * half + plain_row, plain_row, t // 16, 1.0)
        mine = part < 3
        low = jnp.logical_or(part == 2, jnp.logical_and(part == 4, own == 1))
        row = first + jnp.where(low, 256, 0)
        column = jnp.where(mine, jnp.minimum(part, 1), jnp.where(part == 3, own, 1))
        weight = jnp.where(jnp.logical_or(part == 0, part == 2), 0.5, 1.0)
        chosen = (
            CHUNK * jnp.where(mine, own, other) + row,
            CHUNK * jnp.where(mine, 1, 0) + row,
            column,
            weight,
        )
        return [jnp.where(diagonal, a, b) for a, b in zip(chosen, plain)]

    def generate(t, slot):
        cos_row, _, column, _ = tile(t)
        cos_row = pl.multiple_of(cos_row, ROWS)
        column = pl.multiple_of(column * COLS, COLS)
        for first in range(0, ROWS, 16):
            x = cos_ref[pl.ds(cos_row + first, 16), pl.ds(column, COLS)]
            for which, value in factors(x):
                slot[which, first : first + 16] = value
                yield

    def stage(t):
        column = tile(t)[2]
        right = weights[pl.ds(pl.multiple_of(column * COLS, COLS), COLS)]
        for unit in range(2):
            pltpu.matmul_push_rhs(right, 0, unit)

    def left_of(t):
        _, map_row, _, weight = tile(t)
        return maps[pl.ds(pl.multiple_of(map_row, ROWS), ROWS)].astype(f32) * weight

    def sum_of(k):
        unit, turn = k % 2, k // 2
        return sums[unit][turn % 16 if turn < 32 else 16]

    def take(k, left):
        product = pltpu.matmul_pop(sum_of(k)) * left
        total[k + 1] += jnp.sum(product.reshape(ROWS // 8, 8, LANES), axis=0)

    def process(t, now, later):
        following = jnp.minimum(t + 1, count - 1)
        making = generate(following, later)
        left = left_of(jnp.maximum(t - 1, 0))
        for k in range(TOP):
            take((k - LAG) % TOP, left)
            if k == LAG - 1:
                left = left_of(t)
            pltpu.matmul_acc_lhs(
                sum_of(k), basis_function(k, now), load_staged_rhs=0 if k < 2 else None
            )
            if k == 8:
                stage(following)
            next(making, None)
        for _ in making:
            pass

    for one in sums[0] + sums[1]:
        pltpu.matmul_pop(one)
    for _ in generate(0, even):
        pass
    stage(0)

    def step(pair, carry):
        process(2 * pair, even, odd)
        process(2 * pair + 1, odd, even)
        return carry

    lax.fori_loop(0, count // 2, step, 0)
    left = left_of(count - 1)
    for k in range(TOP - LAG, TOP):
        take(k, left)
    for unit in range(2):
        pltpu.matmul_acc_lhs(sums[unit][0], jnp.zeros((ROWS, COLS), bf16), load_staged_rhs=0)
        pltpu.matmul_pop(sums[unit][0])

    spectra = jnp.zeros((L, LANES), f32)
    for k in range(TOP + 1):
        spectra += basis_ref[:, k : k + 1] * jnp.sum(total[k], axis=0, keepdims=True)
    out_ref[...] = spectra[:, :MAPS]


def assemble_kernel(place_ref, half_ref, other_ref, out_ref, scratch):
    r, c = place_ref[0], place_ref[1]
    half = jnp.where(c // 2 > r, c % 2, 1 - c % 2)
    scratch[pl.ds(pl.multiple_of(CHUNK * half, CHUNK), CHUNK)] = half_ref[...]
    scratch[pl.ds(pl.multiple_of(CHUNK * (1 - half), CHUNK), CHUNK)] = other_ref[...]
    out_ref[...] = scratch[...].T


SMEM = pl.BlockSpec(memory_space=pltpu.SMEM)
VMEM = pl.BlockSpec(memory_space=pltpu.VMEM)


def block_spectra(place, cosines, rows, cols):
    return pl.pallas_call(
        spectra_kernel,
        out_shape=(pltpu.VMEM((L, MAPS), f32), pltpu.VMEM((CHUNK, MAPS), bf16)),
        in_specs=[SMEM] + [VMEM] * 10,
        out_specs=(VMEM, VMEM),
        scratch_shapes=[
            pltpu.VMEM((2 * CHUNK, LANES), bf16),
            pltpu.VMEM((CHUNK, LANES), bf16),
            pltpu.VMEM((FACTORS, ROWS, COLS), bf16),
            pltpu.VMEM((FACTORS, ROWS, COLS), bf16),
            pltpu.VMEM((TOP + 1, 8, LANES), f32),
        ],
        cost_estimate=pl.CostEstimate(flops=9 * 10**9, bytes_accessed=4 * 10**6, transcendentals=0),
        compiler_params=pltpu.CompilerParams(
            vmem_limit_bytes=24 * 2**20,
        ),
        name="spectra",
    )(place, cosines, *rows, *cols, jnp.asarray(BASIS))


def assemble(place, half, other):
    return pl.pallas_call(
        assemble_kernel,
        out_shape=jax.ShapeDtypeStruct((MAPS, 2 * CHUNK), bf16),
        in_specs=[SMEM, VMEM, VMEM],
        out_specs=VMEM,
        scratch_shapes=[pltpu.VMEM((2 * CHUNK, MAPS), bf16)],
        compiler_params=pltpu.CompilerParams(vmem_limit_bytes=8 * 2**20),
        name="assemble",
    )(place, half, other).T


def everywhere(value):
    value = value + lax.ppermute(value, PROW[1], [(0, 1), (1, 0)])
    for axis in (PROW[0],) + PCOL:
        near, far, across = (
            lax.ppermute(value, axis, [(i, i ^ mask) for i in range(4)]) for mask in (1, 3, 2)
        )
        value = (value + across) + (near + far)
    return value


def per_device(inverse_cov, cosines, sky_maps):
    place = jnp.stack([lax.axis_index(PROW), lax.axis_index(PCOL)]).astype(jnp.int32)
    partial = jnp.dot(inverse_cov, sky_maps, preferred_element_type=f32)
    partial = with_layout_constraint(partial.astype(f16), Layout(major_to_minor=(0, 1)))
    partial = partial.reshape(NC, PIECE, MAPS)
    parts = lax.all_to_all(partial, ALL, 0, 0, axis_index_groups=SUMMERS, tiled=True)
    piece = jnp.sum(parts.astype(f32), axis=0).astype(bf16)

    cols, rows = lax.ppermute(piece, ALL, TO_COLUMNS)[None], piece[None]
    rows = jnp.concatenate([rows, lax.ppermute(rows, ALL, ROW_STEPS[0])])
    cols = jnp.concatenate([cols, lax.ppermute(cols, ALL, COLUMN_STEPS[0])])
    rows = [rows] + [lax.ppermute(rows, ALL, pairs) for pairs in ROW_STEPS[1:]]
    cols = [cols] + [lax.ppermute(cols, ALL, pairs) for pairs in COLUMN_STEPS[1:]]

    cosines = pltpu.with_memory_space_constraint(cosines, pltpu.VMEM)
    share, half = block_spectra(place, cosines, rows, cols)
    other = lax.ppermute(half, ALL, OTHER_HALF)
    spectra = everywhere(share)
    return assemble(place, half, other), spectra


def solution(mesh):
    split = Mesh(mesh.devices.reshape(4, 2, 4, 4), ALL)
    placed = (P(PROW, PCOL), P(PROW, PCOL), P(PCOL, None))
    return jax.shard_map(
        per_device, mesh=split, in_specs=placed, out_specs=(P(PROW, None), P()), check_vma=False
    )
```

```python
import functools

import jax
import jax.numpy as jnp
import numpy as np
from jax import lax
from jax.experimental import pallas as pl
from jax.experimental.layout import Layout, with_layout_constraint
from jax.experimental.pallas import tpu as pltpu
from jax.sharding import Mesh
from jax.sharding import PartitionSpec as P

NPIX = 8192
MAPS = 192
L = 64
LMIN = 2
TOP = LMIN + L - 1
NR, NC = 8, 16
CHUNK = NPIX // NC
PIECE = CHUNK // NR
LANES = 256
ROWS = 32
COLS = 256
LOW = 9
CENTRES = (18, 37, 56)
CENTRE = 2 * LOW - 1
FACTORS = CENTRE + 2 * len(CENTRES)
LENT = 4
LENT_ROW = 256
LAG = 28
PROW = ("prow_0", "prow_1")
PCOL = ("pcol_0", "pcol_1")
ALL = PROW + PCOL
bf16, f16, f32 = jnp.bfloat16, jnp.float16, jnp.float32
MASKS = (1, 2, 6, 4)
ORDER = (0, 1, 2, 3, 6, 7, 4, 5)


def half_of(r, c):
    return c % 2 if c // 2 > r else 1 - c % 2


def keeper_of(g, y):
    return 2 * ((2 * y + 2 - g // 2) % 4) + g % 2


MEMBERS = [
    [[c for c in range(NC) if half_of(r, c) == s] for s in range(2)] for r in range(NR)
]
EACH = [(r, s, g) for r in range(NR) for s in range(2) for g in range(NR)]
TO_COLUMNS = [
    (r * NC + MEMBERS[r][s][g], keeper_of(g, r // 2) * NC + 2 * r + s) for r, s, g in EACH
]
OTHER_HALF = [(r * NC + MEMBERS[r][s][g], r * NC + MEMBERS[r][1 - s][g]) for r, s, g in EACH]
SUMMERS = [[r * NC + MEMBERS[r][s][g] for s in range(2) for g in range(NR)] for r in range(NR)]
ROW_STEPS = [
    [(r * NC + MEMBERS[r][s][g], r * NC + MEMBERS[r][s][g ^ mask]) for r, s, g in EACH]
    for mask in MASKS
]
COLUMN_STEPS = [
    [(r * NC + c, (r ^ mask) * NC + c) for r in range(NR) for c in range(NC)] for mask in MASKS
]


def basis_matrix():
    g = [1.0]
    for k in range(1, TOP + 1):
        g.append(g[-1] * (2 * k - 1) / (2 * k))
    cheb = np.zeros((L, TOP + 1))
    for row in range(L):
        degree = row + LMIN
        for k in range(degree + 1):
            cheb[row, abs(degree - 2 * k)] += g[k] * g[degree - k]
        cheb[row] *= 2.0 * (2.0 * degree + 1.0) / NPIX
    columns = [cheb[:, k] for k in range(LOW)]
    for n in CENTRES:
        columns.append(cheb[:, n])
        columns += [cheb[:, n - a] + cheb[:, n + a] for a in range(1, LOW + 1)]
        columns += [cheb[:, n - a] - cheb[:, n + a] for a in range(1, LOW + 1)]
    matrix = np.stack(columns, axis=1)
    assert matrix.shape == (L, TOP + 1)
    return matrix.astype(np.float32)


BASIS = basis_matrix()


def factors(x):
    y = x + x
    t, u = [jnp.ones_like(x), x], [jnp.ones_like(x), y]
    yield 0, x.astype(bf16)
    yield LOW, y.astype(bf16)
    for k in range(2, LOW + 1):
        t.append(y * t[k - 1] - t[k - 2])
        yield k - 1, t[k].astype(bf16)
        if k < LOW:
            u.append(y * u[k - 1] - u[k - 2])
            yield LOW + k - 1, u[k].astype(bf16)
    t9, u8 = t[9], u[8]
    square = 1.0 - x * x
    double = t9 + t9
    t18, u17 = double * t9 - 1.0, double * u8
    v18 = square * u17
    yield CENTRE, t18.astype(bf16)
    yield CENTRE + 1, v18.astype(bf16)
    double = t18 + t18
    t36, v36 = double * t18 - 1.0, double * v18
    t37, v37 = t36 * x - v36, v36 * x + t36 * square
    yield CENTRE + 2, t37.astype(bf16)
    yield CENTRE + 3, v37.astype(bf16)
    t19, u18 = t18 * x - v18, u17 * x + t18
    v19 = square * u18
    t56, v56 = t37 * t19 - v37 * u18, v37 * t19 + t37 * v19
    yield CENTRE + 4, t56.astype(bf16)
    yield CENTRE + 5, v56.astype(bf16)


def basis_function(k, made):
    if k < LOW - 1:
        return made[k]
    centre, which = divmod(k - (LOW - 1), 2 * LOW + 1)
    tn, vn = CENTRE + 2 * centre, CENTRE + 2 * centre + 1
    if which == 0:
        return made[tn]
    if which <= LOW:
        return made[tn] * made[which - 1]
    if which == LOW + 1:
        return made[vn]
    return made[vn] * made[LOW + which - LOW - 2]


def spectra_kernel(
    place_ref, cos_ref, lent_ref, r0, r1, r2, r3, c0, c1, c2, c3, basis_ref, out_ref, half_ref,
    maps, weights, even, odd, total,
):
    def with_sums(*sums):
        spectra_body(
            place_ref, cos_ref, lent_ref, (r0, r1, r2, r3), (c0, c1, c2, c3), basis_ref, out_ref, half_ref,
            maps, weights, even, odd, total, (sums[:17], sums[17:]),
        )

    pl.run_scoped(
        with_sums,
        *[pltpu.ACC(0)((ROWS, LANES), f32)] * 17,
        *[pltpu.ACC(1)((ROWS, LANES), f32)] * 16,
    )


def pieces_of(refs):
    return [(ref, at) for ref in refs for at in range(ref.shape[0])]


def spectra_body(
    place_ref, cos_ref, lent_ref, rows_refs, cols_refs, basis_ref, out_ref, half_ref,
    maps, weights, even, odd, total, sums,
):
    r, c = place_ref[0], place_ref[1]
    group, own = c // 2, c % 2
    other = 1 - own
    diagonal = group == r
    half = jnp.where(group > r, own, other)
    zeros = jnp.zeros((PIECE, LANES - MAPS), bf16)
    row_sum = col_sum = jnp.zeros((8, LANES), f32)
    for order, (rows_ref, at), (cols_ref, _) in zip(ORDER, pieces_of(rows_refs), pieces_of(cols_refs)):
        rows = jnp.concatenate([rows_ref[at], zeros], axis=1)
        to = pl.multiple_of((group ^ order) * PIECE, PIECE)
        maps[pl.ds(to, PIECE)] = rows
        half_ref[pl.ds(to, PIECE)] = rows_ref[at]
        cols = jnp.concatenate([cols_ref[at], zeros], axis=1)
        to = pl.multiple_of(keeper_of(r ^ order, c // 4) * PIECE, PIECE)
        weights[pl.ds(to, PIECE)] = cols
        maps[pl.ds(CHUNK + to, PIECE)] = cols
        row_sum += jnp.sum(rows.astype(f32).reshape(PIECE // 8, 8, LANES), axis=0)
        col_sum += jnp.sum(cols.astype(f32).reshape(PIECE // 8, 8, LANES), axis=0)
    row_sum = jnp.sum(row_sum, axis=0, keepdims=True)
    col_sum = jnp.sum(col_sum, axis=0, keepdims=True)
    alpha = jnp.where(diagonal, 0.5, 1.0)
    beta = jnp.where(diagonal, 0.5, 0.0)
    total[...] = jnp.zeros_like(total)
    total[0, 0:1] = col_sum * (alpha * row_sum + beta * col_sum)
    helper = group == r ^ 1
    count = jnp.where(jnp.logical_or(diagonal, helper), 32 + LENT, 32)

    def tile(t):
        part, first = t // 8, 32 * (t % 8)
        plain_row = 32 * (t % 16)
        lent = jnp.logical_and(helper, t >= 32)
        plain = (
            jnp.where(lent, 32 * (t - 32), CHUNK * half + plain_row),
            jnp.where(lent, LENT_ROW + CHUNK + 32 * (t - 32), plain_row),
            jnp.where(lent, 1, t // 16),
            jnp.where(lent, 0.5, 1.0),
        )
        kept = jnp.where(t >= 16, t + LENT, t)
        part, first = kept // 8, 32 * (kept % 8)
        mine = part < 3
        low = jnp.logical_or(part == 2, jnp.logical_and(part == 4, own == 1))
        row = first + jnp.where(low, LENT_ROW, 0)
        column = jnp.where(mine, jnp.minimum(part, 1), jnp.where(part == 3, own, 1))
        weight = jnp.where(jnp.logical_or(part == 0, part == 2), 0.5, 1.0)
        chosen = (
            CHUNK * jnp.where(mine, own, other) + row,
            CHUNK * jnp.where(mine, 1, 0) + row,
            column,
            weight,
        )
        return [jnp.where(diagonal, a, b) for a, b in zip(chosen, plain)] + [lent]

    def generate(t, slot):
        cos_row, _, column, _, lent = tile(t)
        cos_row = pl.multiple_of(cos_row, ROWS)
        lent_row = pl.multiple_of(jnp.where(lent, cos_row, 0), ROWS)
        column = pl.multiple_of(column * COLS, COLS)
        for first in range(0, ROWS, 16):
            x = cos_ref[pl.ds(cos_row + first, 16), pl.ds(column, COLS)]
            x = jnp.where(lent, lent_ref[pl.ds(lent_row + first, 16)], x)
            for which, value in factors(x):
                slot[which, first : first + 16] = value
                yield

    def stage(t):
        column = tile(t)[2]
        right = weights[pl.ds(pl.multiple_of(column * COLS, COLS), COLS)]
        for unit in range(2):
            pltpu.matmul_push_rhs(right, 0, unit)

    def left_of(t):
        _, map_row, _, weight, _ = tile(t)
        return maps[pl.ds(pl.multiple_of(map_row, ROWS), ROWS)].astype(f32) * weight

    def sum_of(k):
        unit, turn = k % 2, k // 2
        return sums[unit][turn % 16 if turn < 32 else 16]

    def take(k, left):
        product = pltpu.matmul_pop(sum_of(k)) * left
        total[k + 1] += jnp.sum(product.reshape(ROWS // 8, 8, LANES), axis=0)

    def process(t, now, later):
        following = jnp.minimum(t + 1, count - 1)
        making = generate(following, later)
        left = left_of(jnp.maximum(t - 1, 0))
        for k in range(TOP):
            take((k - LAG) % TOP, left)
            if k == LAG - 1:
                left = left_of(t)
            pltpu.matmul_acc_lhs(
                sum_of(k), basis_function(k, now), load_staged_rhs=0 if k < 2 else None
            )
            if k == 8:
                stage(following)
            next(making, None)
        for _ in making:
            pass

    for one in sums[0] + sums[1]:
        pltpu.matmul_pop(one)
    for _ in generate(0, even):
        pass
    stage(0)

    def step(pair, carry):
        process(2 * pair, even, odd)
        process(2 * pair + 1, odd, even)
        return carry

    lax.fori_loop(0, count // 2, step, 0)
    left = left_of(count - 1)
    for k in range(TOP - LAG, TOP):
        take(k, left)
    for unit in range(2):
        pltpu.matmul_acc_lhs(sums[unit][0], jnp.zeros((ROWS, COLS), bf16), load_staged_rhs=0)
        pltpu.matmul_pop(sums[unit][0])

    spectra = jnp.zeros((L, LANES), f32)
    for k in range(TOP + 1):
        spectra += basis_ref[:, k : k + 1] * jnp.sum(total[k], axis=0, keepdims=True)
    out_ref[...] = spectra[:, :MAPS]


def assemble_kernel(place_ref, half_ref, other_ref, out_ref, scratch):
    r, c = place_ref[0], place_ref[1]
    half = jnp.where(c // 2 > r, c % 2, 1 - c % 2)
    scratch[pl.ds(pl.multiple_of(CHUNK * half, CHUNK), CHUNK)] = half_ref[...]
    scratch[pl.ds(pl.multiple_of(CHUNK * (1 - half), CHUNK), CHUNK)] = other_ref[...]
    out_ref[...] = scratch[...].T


SMEM = pl.BlockSpec(memory_space=pltpu.SMEM)
VMEM = pl.BlockSpec(memory_space=pltpu.VMEM)


def block_spectra(place, cosines, lent, rows, cols):
    return pl.pallas_call(
        spectra_kernel,
        out_shape=(pltpu.VMEM((L, MAPS), f32), pltpu.VMEM((CHUNK, MAPS), bf16)),
        in_specs=[SMEM] + [VMEM] * 11,
        out_specs=(VMEM, VMEM),
        scratch_shapes=[
            pltpu.VMEM((2 * CHUNK, LANES), bf16),
            pltpu.VMEM((CHUNK, LANES), bf16),
            pltpu.VMEM((FACTORS, ROWS, COLS), bf16),
            pltpu.VMEM((FACTORS, ROWS, COLS), bf16),
            pltpu.VMEM((TOP + 1, 8, LANES), f32),
        ],
        cost_estimate=pl.CostEstimate(flops=9 * 10**9, bytes_accessed=4 * 10**6, transcendentals=0),
        compiler_params=pltpu.CompilerParams(
            vmem_limit_bytes=24 * 2**20,
        ),
        name="spectra",
    )(place, cosines, lent, *rows, *cols, jnp.asarray(BASIS))


def assemble(place, half, other):
    return pl.pallas_call(
        assemble_kernel,
        out_shape=jax.ShapeDtypeStruct((MAPS, 2 * CHUNK), bf16),
        in_specs=[SMEM, VMEM, VMEM],
        out_specs=VMEM,
        scratch_shapes=[pltpu.VMEM((2 * CHUNK, MAPS), bf16)],
        compiler_params=pltpu.CompilerParams(vmem_limit_bytes=8 * 2**20),
        name="assemble",
    )(place, half, other).T


def everywhere(value):
    value = value + lax.ppermute(value, PROW[1], [(0, 1), (1, 0)])
    for axis in (PROW[0],) + PCOL:
        near, far, across = (
            lax.ppermute(value, axis, [(i, i ^ mask) for i in range(4)]) for mask in (1, 3, 2)
        )
        value = (value + across) + (near + far)
    return value


def per_device(inverse_cov, cosines, sky_maps):
    place = jnp.stack([lax.axis_index(PROW), lax.axis_index(PCOL)]).astype(jnp.int32)
    lent = lax.dynamic_slice(
        cosines, (CHUNK * (place[1] % 2) + LENT_ROW, COLS), (LENT * ROWS, COLS)
    )
    lent, sky_maps = lax.optimization_barrier((lent, sky_maps))
    lent = lax.ppermute(lent, PROW[1], [(0, 1), (1, 0)])
    partial = jnp.dot(inverse_cov, sky_maps, preferred_element_type=f32)
    partial = with_layout_constraint(partial.astype(f16), Layout(major_to_minor=(0, 1)))
    partial = partial.reshape(NC, PIECE, MAPS)
    parts = lax.all_to_all(partial, ALL, 0, 0, axis_index_groups=SUMMERS, tiled=True)
    piece = jnp.sum(parts.astype(f32), axis=0).astype(bf16)

    cols, rows = lax.ppermute(piece, ALL, TO_COLUMNS)[None], piece[None]
    rows = jnp.concatenate([rows, lax.ppermute(rows, ALL, ROW_STEPS[0])])
    cols = jnp.concatenate([cols, lax.ppermute(cols, ALL, COLUMN_STEPS[0])])
    rows = [rows] + [lax.ppermute(rows, ALL, pairs) for pairs in ROW_STEPS[1:]]
    cols = [cols] + [lax.ppermute(cols, ALL, pairs) for pairs in COLUMN_STEPS[1:]]

    cosines = pltpu.with_memory_space_constraint(cosines, pltpu.VMEM)
    share, half = block_spectra(place, cosines, lent, rows, cols)
    other = lax.ppermute(half, ALL, OTHER_HALF)
    spectra = everywhere(share)
    return assemble(place, half, other), spectra


def solution(mesh):
    split = Mesh(mesh.devices.reshape(4, 2, 4, 4), ALL)
    placed = (P(PROW, PCOL), P(PROW, PCOL), P(PCOL, None))
    return jax.shard_map(
        per_device, mesh=split, in_specs=placed, out_specs=(P(PROW, None), P()), check_vma=False
    )
```

```python
import functools

import jax
import jax.numpy as jnp
import numpy as np
from jax import lax
from jax.experimental import pallas as pl
from jax.experimental.pallas import tpu as pltpu
from jax.sharding import Mesh
from jax.sharding import PartitionSpec as P

NPIX = 8192
MAPS = 192
L = 64
LMIN = 2
TOP = LMIN + L - 1
NR, NC = 8, 16
CHUNK = NPIX // NC
PIECE = CHUNK // NR
LANES = 256
LANE = 128
SENT = PIECE * MAPS // LANE
ROWS = 32
COLS = 256
LOW = 9
CENTRES = (18, 37, 56)
CENTRE = 2 * LOW - 1
FACTORS = CENTRE + 2 * len(CENTRES)
LENT = 4
LENT_ROW = 256
LAG = 28
PROW = ("prow_0", "prow_1")
PCOL = ("pcol_0", "pcol_1")
ALL = PROW + PCOL
bf16, f16, f32 = jnp.bfloat16, jnp.float16, jnp.float32
MASKS = (1, 2, 6, 4)
ORDER = (0, 1, 2, 3, 6, 7, 4, 5)


def half_of(r, c):
    return c % 2 if c // 2 > r else 1 - c % 2


def keeper_of(g, y):
    return 2 * ((2 * y + 2 - g // 2) % 4) + g % 2


MEMBERS = [
    [[c for c in range(NC) if half_of(r, c) == s] for s in range(2)] for r in range(NR)
]
EACH = [(r, s, g) for r in range(NR) for s in range(2) for g in range(NR)]
TO_COLUMNS = [
    (r * NC + MEMBERS[r][s][g], keeper_of(g, r // 2) * NC + 2 * r + s) for r, s, g in EACH
]
OTHER_HALF = [(r * NC + MEMBERS[r][s][g], r * NC + MEMBERS[r][1 - s][g]) for r, s, g in EACH]
SUMMERS = [[r * NC + MEMBERS[r][s][g] for s in range(2) for g in range(NR)] for r in range(NR)]
ROW_STEPS = [
    [(r * NC + MEMBERS[r][s][g], r * NC + MEMBERS[r][s][g ^ mask]) for r, s, g in EACH]
    for mask in MASKS
]
COLUMN_STEPS = [
    [(r * NC + c, (r ^ mask) * NC + c) for r in range(NR) for c in range(NC)] for mask in MASKS
]


def basis_matrix():
    g = [1.0]
    for k in range(1, TOP + 1):
        g.append(g[-1] * (2 * k - 1) / (2 * k))
    cheb = np.zeros((L, TOP + 1))
    for row in range(L):
        degree = row + LMIN
        for k in range(degree + 1):
            cheb[row, abs(degree - 2 * k)] += g[k] * g[degree - k]
        cheb[row] *= 2.0 * (2.0 * degree + 1.0) / NPIX
    columns = [cheb[:, k] for k in range(LOW)]
    for n in CENTRES:
        columns.append(cheb[:, n])
        columns += [cheb[:, n - a] + cheb[:, n + a] for a in range(1, LOW + 1)]
        columns += [cheb[:, n - a] - cheb[:, n + a] for a in range(1, LOW + 1)]
    matrix = np.stack(columns, axis=1)
    assert matrix.shape == (L, TOP + 1)
    return matrix.astype(np.float32)


BASIS = basis_matrix()


def factors(x):
    y = x + x
    t, u = [jnp.ones_like(x), x], [jnp.ones_like(x), y]
    yield 0, x.astype(bf16)
    yield LOW, y.astype(bf16)
    for k in range(2, LOW + 1):
        t.append(y * t[k - 1] - t[k - 2])
        yield k - 1, t[k].astype(bf16)
        if k < LOW:
            u.append(y * u[k - 1] - u[k - 2])
            yield LOW + k - 1, u[k].astype(bf16)
    t9, u8 = t[9], u[8]
    square = 1.0 - x * x
    double = t9 + t9
    t18, u17 = double * t9 - 1.0, double * u8
    v18 = square * u17
    yield CENTRE, t18.astype(bf16)
    yield CENTRE + 1, v18.astype(bf16)
    double = t18 + t18
    t36, v36 = double * t18 - 1.0, double * v18
    t37, v37 = t36 * x - v36, v36 * x + t36 * square
    yield CENTRE + 2, t37.astype(bf16)
    yield CENTRE + 3, v37.astype(bf16)
    t19, u18 = t18 * x - v18, u17 * x + t18
    v19 = square * u18
    t56, v56 = t37 * t19 - v37 * u18, v37 * t19 + t37 * v19
    yield CENTRE + 4, t56.astype(bf16)
    yield CENTRE + 5, v56.astype(bf16)


def basis_function(k, made):
    if k < LOW - 1:
        return made[k]
    centre, which = divmod(k - (LOW - 1), 2 * LOW + 1)
    tn, vn = CENTRE + 2 * centre, CENTRE + 2 * centre + 1
    if which == 0:
        return made[tn]
    if which <= LOW:
        return made[tn] * made[which - 1]
    if which == LOW + 1:
        return made[vn]
    return made[vn] * made[LOW + which - LOW - 2]


def unpacked(piece):
    rest = piece[PIECE:].astype(f32)
    first = lax.broadcasted_iota(jnp.int32, rest.shape, 1) < LANE // 2
    upper = jnp.where(first, rest, 0.0)
    lower = jnp.where(first, pltpu.roll(rest, LANE // 2, 1), 0.0)
    rest = jnp.concatenate([upper, lower], axis=0).astype(piece.dtype)
    return jnp.concatenate([piece[:PIECE], rest], axis=1)


def partial_kernel(cov_ref, maps_ref, upper_ref, lower_ref, out_ref, lent_ref):
    lent_ref[0] = upper_ref[...]
    lent_ref[1] = lower_ref[...]
    zeros = jnp.zeros((LANES - MAPS, maps_ref.shape[1]), bf16)
    maps = jnp.concatenate([maps_ref[...], zeros], axis=0)
    product = lax.dot_general(
        cov_ref[...], maps, (((1,), (1,)), ((), ())), preferred_element_type=f32
    )
    for piece in range(NC):
        rows = product[PIECE * piece : PIECE * (piece + 1)]
        out_ref[piece, :PIECE] = rows[:, :LANE]
        rest = rows[:, LANE:]
        out_ref[piece, PIECE:] = rest[: PIECE // 2] + pltpu.roll(rest[PIECE // 2 :], LANE // 2, 1)


def spectra_kernel(
    place_ref, cos_ref, lent_ref, r0, r1, r2, r3, c0, c1, c2, c3, basis_ref, out_ref, half_ref,
    maps, weights, even, odd, total,
):
    def with_sums(*sums):
        spectra_body(
            place_ref, cos_ref, lent_ref, (r0, r1, r2, r3), (c0, c1, c2, c3), basis_ref, out_ref, half_ref,
            maps, weights, even, odd, total, (sums[:17], sums[17:]),
        )

    pl.run_scoped(
        with_sums,
        *[pltpu.ACC(0)((ROWS, LANES), f32)] * 17,
        *[pltpu.ACC(1)((ROWS, LANES), f32)] * 16,
    )


def pieces_of(refs):
    return [(ref, at) for ref in refs for at in range(ref.shape[0])]


def spectra_body(
    place_ref, cos_ref, lent_ref, rows_refs, cols_refs, basis_ref, out_ref, half_ref,
    maps, weights, even, odd, total, sums,
):
    r, c = place_ref[0], place_ref[1]
    group, own = c // 2, c % 2
    other = 1 - own
    diagonal = group == r
    half = jnp.where(group > r, own, other)
    row_sum = col_sum = jnp.zeros((8, LANES), f32)
    for order, (rows_ref, at), (cols_ref, _) in zip(ORDER, pieces_of(rows_refs), pieces_of(cols_refs)):
        rows = unpacked(rows_ref[at])
        to = pl.multiple_of((group ^ order) * PIECE, PIECE)
        maps[pl.ds(to, PIECE)] = rows
        half_ref[group ^ order] = rows_ref[at]
        cols = unpacked(cols_ref[at])
        to = pl.multiple_of(keeper_of(r ^ order, c // 4) * PIECE, PIECE)
        weights[pl.ds(to, PIECE)] = cols
        maps[pl.ds(CHUNK + to, PIECE)] = cols
        row_sum += jnp.sum(rows.astype(f32).reshape(PIECE // 8, 8, LANES), axis=0)
        col_sum += jnp.sum(cols.astype(f32).reshape(PIECE // 8, 8, LANES), axis=0)
    row_sum = jnp.sum(row_sum, axis=0, keepdims=True)
    col_sum = jnp.sum(col_sum, axis=0, keepdims=True)
    alpha = jnp.where(diagonal, 0.5, 1.0)
    beta = jnp.where(diagonal, 0.5, 0.0)
    total[...] = jnp.zeros_like(total)
    total[0, 0:1] = col_sum * (alpha * row_sum + beta * col_sum)
    helper = group == r ^ 1
    count = jnp.where(jnp.logical_or(diagonal, helper), 32 + LENT, 32)

    def tile(t):
        part, first = t // 8, 32 * (t % 8)
        plain_row = 32 * (t % 16)
        lent = jnp.logical_and(helper, t >= 32)
        plain = (
            jnp.where(lent, 32 * (t - 32), CHUNK * half + plain_row),
            jnp.where(lent, LENT_ROW + CHUNK + 32 * (t - 32), plain_row),
            jnp.where(lent, 1, t // 16),
            jnp.where(lent, 0.5, 1.0),
        )
        kept = jnp.where(t >= 16, t + LENT, t)
        part, first = kept // 8, 32 * (kept % 8)
        mine = part < 3
        low = jnp.logical_or(part == 2, jnp.logical_and(part == 4, own == 1))
        row = first + jnp.where(low, LENT_ROW, 0)
        column = jnp.where(mine, jnp.minimum(part, 1), jnp.where(part == 3, own, 1))
        weight = jnp.where(jnp.logical_or(part == 0, part == 2), 0.5, 1.0)
        chosen = (
            CHUNK * jnp.where(mine, own, other) + row,
            CHUNK * jnp.where(mine, 1, 0) + row,
            column,
            weight,
        )
        return [jnp.where(diagonal, a, b) for a, b in zip(chosen, plain)] + [lent]

    def generate(t, slot):
        cos_row, _, column, _, lent = tile(t)
        cos_row = pl.multiple_of(cos_row, ROWS)
        lent_row = pl.multiple_of(jnp.where(lent, cos_row, 0), ROWS)
        column = pl.multiple_of(column * COLS, COLS)
        for first in range(0, ROWS, 16):
            x = cos_ref[pl.ds(cos_row + first, 16), pl.ds(column, COLS)]
            x = jnp.where(lent, lent_ref[own, pl.ds(lent_row + first, 16)], x)
            for which, value in factors(x):
                slot[which, first : first + 16] = value
                yield

    def stage(t):
        column = tile(t)[2]
        right = weights[pl.ds(pl.multiple_of(column * COLS, COLS), COLS)]
        for unit in range(2):
            pltpu.matmul_push_rhs(right, 0, unit)

    def left_of(t):
        _, map_row, _, weight, _ = tile(t)
        return maps[pl.ds(pl.multiple_of(map_row, ROWS), ROWS)].astype(f32) * weight

    def sum_of(k):
        unit, turn = k % 2, k // 2
        return sums[unit][turn % 16 if turn < 32 else 16]

    def take(k, left):
        product = pltpu.matmul_pop(sum_of(k)) * left
        total[k + 1] += jnp.sum(product.reshape(ROWS // 8, 8, LANES), axis=0)

    def process(t, now, later):
        following = jnp.minimum(t + 1, count - 1)
        making = generate(following, later)
        left = left_of(jnp.maximum(t - 1, 0))
        for k in range(TOP):
            take((k - LAG) % TOP, left)
            if k == LAG - 1:
                left = left_of(t)
            pltpu.matmul_acc_lhs(
                sum_of(k), basis_function(k, now), load_staged_rhs=0 if k < 2 else None
            )
            if k == 8:
                stage(following)
            next(making, None)
        for _ in making:
            pass

    for one in sums[0] + sums[1]:
        pltpu.matmul_pop(one)
    for _ in generate(0, even):
        pass
    stage(0)

    def step(pair, carry):
        process(2 * pair, even, odd)
        process(2 * pair + 1, odd, even)
        return carry

    lax.fori_loop(0, count // 2, step, 0)
    left = left_of(count - 1)
    for k in range(TOP - LAG, TOP):
        take(k, left)
    for unit in range(2):
        pltpu.matmul_acc_lhs(sums[unit][0], jnp.zeros((ROWS, COLS), bf16), load_staged_rhs=0)
        pltpu.matmul_pop(sums[unit][0])

    spectra = jnp.zeros((L, LANES), f32)
    for k in range(TOP + 1):
        spectra += basis_ref[:, k : k + 1] * jnp.sum(total[k], axis=0, keepdims=True)
    out_ref[:L] = spectra[:, :LANE]
    rest = spectra[:, LANE:]
    lane = lax.broadcasted_iota(jnp.int32, (L // 2, LANE), 1)
    out_ref[L:] = jnp.where(lane < LANE // 2, rest[: L // 2], pltpu.roll(rest[L // 2 :], LANE // 2, 1))


def assemble_kernel(place_ref, half_ref, other_ref, out_ref, scratch):
    r, c = place_ref[0], place_ref[1]
    half = jnp.where(c // 2 > r, c % 2, 1 - c % 2)
    for piece in range(NR):
        at = pl.multiple_of(CHUNK * half + PIECE * piece, PIECE)
        scratch[pl.ds(at, PIECE)] = unpacked(half_ref[piece])
        at = pl.multiple_of(CHUNK * (1 - half) + PIECE * piece, PIECE)
        scratch[pl.ds(at, PIECE)] = unpacked(other_ref[piece])
    out_ref[...] = scratch[...][:, :MAPS].T


SMEM = pl.BlockSpec(memory_space=pltpu.SMEM)
VMEM = pl.BlockSpec(memory_space=pltpu.VMEM)


def partial_products(cov, maps, cosines):
    tall = LENT * ROWS
    blocks = [
        pl.BlockSpec((tall, COLS), lambda i, first=first: (first // tall, 1))
        for first in (LENT_ROW, CHUNK + LENT_ROW)
    ]
    whole = [pl.BlockSpec(array.shape, lambda i: (0, 0)) for array in (cov, maps)]
    shapes = (NC, SENT, LANE), (2, tall, COLS)
    return pl.pallas_call(
        partial_kernel,
        grid=(1,),
        out_shape=tuple(pltpu.VMEM(shape, f32) for shape in shapes),
        in_specs=whole + blocks,
        out_specs=tuple(pl.BlockSpec(shape, lambda i: (0, 0, 0)) for shape in shapes),
        compiler_params=pltpu.CompilerParams(vmem_limit_bytes=16 * 2**20),
        name="partial",
    )(cov, maps, cosines, cosines)


def block_spectra(place, cosines, lent, rows, cols):
    return pl.pallas_call(
        spectra_kernel,
        out_shape=(pltpu.VMEM((L + L // 2, LANE), f32), pltpu.VMEM((NR, SENT, LANE), bf16)),
        in_specs=[SMEM] + [VMEM] * 11,
        out_specs=(VMEM, VMEM),
        scratch_shapes=[
            pltpu.VMEM((2 * CHUNK, LANES), bf16),
            pltpu.VMEM((CHUNK, LANES), bf16),
            pltpu.VMEM((FACTORS, ROWS, COLS), bf16),
            pltpu.VMEM((FACTORS, ROWS, COLS), bf16),
            pltpu.VMEM((TOP + 1, 8, LANES), f32),
        ],
        cost_estimate=pl.CostEstimate(flops=9 * 10**9, bytes_accessed=4 * 10**6, transcendentals=0),
        compiler_params=pltpu.CompilerParams(
            vmem_limit_bytes=24 * 2**20,
        ),
        name="spectra",
    )(place, cosines, lent, *rows, *cols, jnp.asarray(BASIS))


def assemble(place, half, other):
    return pl.pallas_call(
        assemble_kernel,
        out_shape=jax.ShapeDtypeStruct((MAPS, 2 * CHUNK), bf16),
        in_specs=[SMEM, VMEM, VMEM],
        out_specs=VMEM,
        scratch_shapes=[pltpu.VMEM((2 * CHUNK, LANES), bf16)],
        compiler_params=pltpu.CompilerParams(vmem_limit_bytes=8 * 2**20),
        name="assemble",
    )(place, half, other).T


def everywhere(value):
    value = value + lax.ppermute(value, PROW[1], [(0, 1), (1, 0)])
    for axis in (PROW[0],) + PCOL:
        near, far, across = (
            lax.ppermute(value, axis, [(i, i ^ mask) for i in range(4)]) for mask in (1, 3, 2)
        )
        value = (value + across) + (near + far)
    return value


def per_device(inverse_cov, cosines, sky_maps):
    place = jnp.stack([lax.axis_index(PROW), lax.axis_index(PCOL)]).astype(jnp.int32)
    inverse_cov, sky_maps, corner = (
        pltpu.with_memory_space_constraint(value, pltpu.HBM)
        for value in (inverse_cov, sky_maps.T, cosines)
    )
    partial, lent = partial_products(inverse_cov, sky_maps, corner)
    partial = partial.astype(f16)
    parts = lax.all_to_all(partial, ALL, 0, 0, axis_index_groups=SUMMERS, tiled=True)
    piece = jnp.sum(parts.astype(f32), axis=0).astype(bf16)
    lent, piece = lax.optimization_barrier((lent, piece))
    lent = lax.ppermute(lent, PROW[1], [(0, 1), (1, 0)])

    cols, rows = lax.ppermute(piece, ALL, TO_COLUMNS)[None], piece[None]
    rows = jnp.concatenate([rows, lax.ppermute(rows, ALL, ROW_STEPS[0])])
    cols = jnp.concatenate([cols, lax.ppermute(cols, ALL, COLUMN_STEPS[0])])
    rows = [rows] + [lax.ppermute(rows, ALL, pairs) for pairs in ROW_STEPS[1:]]
    cols = [cols] + [lax.ppermute(cols, ALL, pairs) for pairs in COLUMN_STEPS[1:]]

    cosines = pltpu.with_memory_space_constraint(cosines, pltpu.VMEM)
    share, half = block_spectra(place, cosines, lent, rows, cols)
    other = lax.ppermute(half, ALL, OTHER_HALF)
    packed = everywhere(share)
    rest = jnp.concatenate([packed[L:, : LANE // 2], packed[L:, LANE // 2 :]], axis=0)
    spectra = jnp.concatenate([packed[:L], rest], axis=1)
    return assemble(place, half, other), spectra


def solution(mesh):
    split = Mesh(mesh.devices.reshape(4, 2, 4, 4), ALL)
    placed = (P(PROW, PCOL), P(PROW, PCOL), P(PCOL, None))
    return jax.shard_map(
        per_device, mesh=split, in_specs=placed, out_specs=(P(PROW, None), P()), check_vma=False
    )
```

```python
import functools

import jax
import jax.numpy as jnp
import numpy as np
from jax import lax
from jax.experimental import pallas as pl
from jax.experimental.pallas import tpu as pltpu
from jax.sharding import Mesh
from jax.sharding import PartitionSpec as P

NPIX = 8192
MAPS = 192
L = 64
LMIN = 2
TOP = LMIN + L - 1
NR, NC = 8, 16
CHUNK = NPIX // NC
PIECE = CHUNK // NR
LANES = 256
LANE = 128
SENT = PIECE * MAPS // LANE
ROWS = 32
COLS = 256
LOW = 9
CENTRES = (18, 37, 56)
CENTRE = 2 * LOW - 1
FACTORS = CENTRE + 2 * len(CENTRES)
LENT = 4
LENT_ROW = 256
LAG = 28
PROW = ("prow_0", "prow_1")
PCOL = ("pcol_0", "pcol_1")
ALL = PROW + PCOL
bf16, f16, f32 = jnp.bfloat16, jnp.float16, jnp.float32
MASKS = (1, 2, 6, 4)
ORDER = (0, 1, 2, 3, 6, 7, 4, 5)


def half_of(r, c):
    return c % 2 if c // 2 > r else 1 - c % 2


def keeper_of(g, y):
    return 2 * ((2 * y + 2 - g // 2) % 4) + g % 2


MEMBERS = [
    [[c for c in range(NC) if half_of(r, c) == s] for s in range(2)] for r in range(NR)
]
EACH = [(r, s, g) for r in range(NR) for s in range(2) for g in range(NR)]
TO_COLUMNS = [
    (r * NC + MEMBERS[r][s][g], keeper_of(g, r // 2) * NC + 2 * r + s) for r, s, g in EACH
]
OTHER_HALF = [(r * NC + MEMBERS[r][s][g], r * NC + MEMBERS[r][1 - s][g]) for r, s, g in EACH]
SUMMERS = [[r * NC + MEMBERS[r][s][g] for s in range(2) for g in range(NR)] for r in range(NR)]
ROW_STEPS = [
    [(r * NC + MEMBERS[r][s][g], r * NC + MEMBERS[r][s][g ^ mask]) for r, s, g in EACH]
    for mask in MASKS
]
COLUMN_STEPS = [
    [(r * NC + c, (r ^ mask) * NC + c) for r in range(NR) for c in range(NC)] for mask in MASKS
]


def basis_matrix():
    g = [1.0]
    for k in range(1, TOP + 1):
        g.append(g[-1] * (2 * k - 1) / (2 * k))
    cheb = np.zeros((L, TOP + 1))
    for row in range(L):
        degree = row + LMIN
        for k in range(degree + 1):
            cheb[row, abs(degree - 2 * k)] += g[k] * g[degree - k]
        cheb[row] *= 2.0 * (2.0 * degree + 1.0) / NPIX
    columns = [cheb[:, k] for k in range(LOW)]
    for n in CENTRES:
        columns.append(cheb[:, n])
        columns += [cheb[:, n - a] + cheb[:, n + a] for a in range(1, LOW + 1)]
        columns += [cheb[:, n - a] - cheb[:, n + a] for a in range(1, LOW + 1)]
    matrix = np.stack(columns, axis=1)
    assert matrix.shape == (L, TOP + 1)
    matrix = matrix.reshape(L // 2, 2, TOP + 1).transpose(1, 0, 2).astype(np.float32)
    parity = [int(not matrix[0, :, k].any()) for k in range(TOP + 1)]
    assert all(not matrix[1 - parity[k], :, k].any() for k in range(TOP + 1))
    return matrix, parity


BASIS, PARITY = basis_matrix()


def factors(x):
    y = x + x
    t, u = [jnp.ones_like(x), x], [jnp.ones_like(x), y]
    yield 0, x.astype(bf16)
    yield LOW, y.astype(bf16)
    for k in range(2, LOW + 1):
        t.append(y * t[k - 1] - t[k - 2])
        yield k - 1, t[k].astype(bf16)
        if k < LOW:
            u.append(y * u[k - 1] - u[k - 2])
            yield LOW + k - 1, u[k].astype(bf16)
    t9, u8 = t[9], u[8]
    square = 1.0 - x * x
    double = t9 + t9
    t18, u17 = double * t9 - 1.0, double * u8
    v18 = square * u17
    yield CENTRE, t18.astype(bf16)
    yield CENTRE + 1, v18.astype(bf16)
    double = t18 + t18
    t36, v36 = double * t18 - 1.0, double * v18
    t37, v37 = t36 * x - v36, v36 * x + t36 * square
    yield CENTRE + 2, t37.astype(bf16)
    yield CENTRE + 3, v37.astype(bf16)
    t19, u18 = t18 * x - v18, u17 * x + t18
    v19 = square * u18
    t56, v56 = t37 * t19 - v37 * u18, v37 * t19 + t37 * v19
    yield CENTRE + 4, t56.astype(bf16)
    yield CENTRE + 5, v56.astype(bf16)


def basis_function(k, made):
    if k < LOW - 1:
        return made[k]
    centre, which = divmod(k - (LOW - 1), 2 * LOW + 1)
    tn, vn = CENTRE + 2 * centre, CENTRE + 2 * centre + 1
    if which == 0:
        return made[tn]
    if which <= LOW:
        return made[tn] * made[which - 1]
    if which == LOW + 1:
        return made[vn]
    return made[vn] * made[LOW + which - LOW - 2]


def unpacked(piece):
    rest = piece[PIECE:].astype(f32)
    first = lax.broadcasted_iota(jnp.int32, rest.shape, 1) < LANE // 2
    upper = jnp.where(first, rest, 0.0)
    lower = jnp.where(first, pltpu.roll(rest, LANE // 2, 1), 0.0)
    rest = jnp.concatenate([upper, lower], axis=0).astype(piece.dtype)
    return jnp.concatenate([piece[:PIECE], rest], axis=1)


def partial_kernel(cov_ref, maps_ref, upper_ref, lower_ref, out_ref, lent_ref):
    lent_ref[0] = upper_ref[...]
    lent_ref[1] = lower_ref[...]
    zeros = jnp.zeros((LANES - MAPS, maps_ref.shape[1]), bf16)
    maps = jnp.concatenate([maps_ref[...], zeros], axis=0)
    product = lax.dot_general(
        cov_ref[...], maps, (((1,), (1,)), ((), ())), preferred_element_type=f32
    )
    for piece in range(NC):
        rows = product[PIECE * piece : PIECE * (piece + 1)]
        out_ref[piece, :PIECE] = rows[:, :LANE]
        rest = rows[:, LANE:]
        out_ref[piece, PIECE:] = rest[: PIECE // 2] + pltpu.roll(rest[PIECE // 2 :], LANE // 2, 1)


def spectra_kernel(
    place_ref, cos_ref, lent_ref, r0, r1, r2, r3, c0, c1, c2, c3, basis_ref, out_ref, half_ref,
    maps, weights, even, odd, total,
):
    def with_sums(*sums):
        spectra_body(
            place_ref, cos_ref, lent_ref, (r0, r1, r2, r3), (c0, c1, c2, c3), basis_ref, out_ref, half_ref,
            maps, weights, even, odd, total, (sums[:17], sums[17:]),
        )

    pl.run_scoped(
        with_sums,
        *[pltpu.ACC(0)((ROWS, LANES), f32)] * 17,
        *[pltpu.ACC(1)((ROWS, LANES), f32)] * 16,
    )


def pieces_of(refs):
    return [(ref, at) for ref in refs for at in range(ref.shape[0])]


def spectra_body(
    place_ref, cos_ref, lent_ref, rows_refs, cols_refs, basis_ref, out_ref, half_ref,
    maps, weights, even, odd, total, sums,
):
    r, c = place_ref[0], place_ref[1]
    group, own = c // 2, c % 2
    other = 1 - own
    diagonal = group == r
    half = jnp.where(group > r, own, other)
    row_sum = col_sum = jnp.zeros((8, LANES), f32)
    for order, (rows_ref, at), (cols_ref, _) in zip(ORDER, pieces_of(rows_refs), pieces_of(cols_refs)):
        rows = unpacked(rows_ref[at])
        to = pl.multiple_of((group ^ order) * PIECE, PIECE)
        maps[pl.ds(to, PIECE)] = rows
        half_ref[group ^ order] = rows_ref[at]
        cols = unpacked(cols_ref[at])
        to = pl.multiple_of(keeper_of(r ^ order, c // 4) * PIECE, PIECE)
        weights[pl.ds(to, PIECE)] = cols
        maps[pl.ds(CHUNK + to, PIECE)] = cols
        row_sum += jnp.sum(rows.astype(f32).reshape(PIECE // 8, 8, LANES), axis=0)
        col_sum += jnp.sum(cols.astype(f32).reshape(PIECE // 8, 8, LANES), axis=0)
    row_sum = jnp.sum(row_sum, axis=0, keepdims=True)
    col_sum = jnp.sum(col_sum, axis=0, keepdims=True)
    alpha = jnp.where(diagonal, 0.5, 1.0)
    beta = jnp.where(diagonal, 0.5, 0.0)
    total[...] = jnp.zeros_like(total)
    total[0, 0:1] = col_sum * (alpha * row_sum + beta * col_sum)
    helper = group == r ^ 1
    count = jnp.where(jnp.logical_or(diagonal, helper), 32 + LENT, 32)

    def tile(t):
        part, first = t // 8, 32 * (t % 8)
        plain_row = 32 * (t % 16)
        lent = jnp.logical_and(helper, t >= 32)
        plain = (
            jnp.where(lent, 32 * (t - 32), CHUNK * half + plain_row),
            jnp.where(lent, LENT_ROW + CHUNK + 32 * (t - 32), plain_row),
            jnp.where(lent, 1, t // 16),
            jnp.where(lent, 0.5, 1.0),
        )
        kept = jnp.where(t >= 16, t + LENT, t)
        part, first = kept // 8, 32 * (kept % 8)
        mine = part < 3
        low = jnp.logical_or(part == 2, jnp.logical_and(part == 4, own == 1))
        row = first + jnp.where(low, LENT_ROW, 0)
        column = jnp.where(mine, jnp.minimum(part, 1), jnp.where(part == 3, own, 1))
        weight = jnp.where(jnp.logical_or(part == 0, part == 2), 0.5, 1.0)
        chosen = (
            CHUNK * jnp.where(mine, own, other) + row,
            CHUNK * jnp.where(mine, 1, 0) + row,
            column,
            weight,
        )
        return [jnp.where(diagonal, a, b) for a, b in zip(chosen, plain)] + [lent]

    def generate(t, slot):
        cos_row, _, column, _, lent = tile(t)
        cos_row = pl.multiple_of(cos_row, ROWS)
        lent_row = pl.multiple_of(jnp.where(lent, cos_row, 0), ROWS)
        column = pl.multiple_of(column * COLS, COLS)
        for first in range(0, ROWS, 16):
            x = cos_ref[pl.ds(cos_row + first, 16), pl.ds(column, COLS)]
            x = jnp.where(lent, lent_ref[own, pl.ds(lent_row + first, 16)], x)
            for which, value in factors(x):
                slot[which, first : first + 16] = value
                yield

    def stage(t):
        column = tile(t)[2]
        right = weights[pl.ds(pl.multiple_of(column * COLS, COLS), COLS)]
        for unit in range(2):
            pltpu.matmul_push_rhs(right, 0, unit)

    def left_of(t):
        _, map_row, _, weight, _ = tile(t)
        return maps[pl.ds(pl.multiple_of(map_row, ROWS), ROWS)].astype(f32) * weight

    def sum_of(k):
        unit, turn = k % 2, k // 2
        return sums[unit][turn % 16 if turn < 32 else 16]

    def take(k, left):
        product = pltpu.matmul_pop(sum_of(k)) * left
        total[k + 1] += jnp.sum(product.reshape(ROWS // 8, 8, LANES), axis=0)

    def process(t, now, later):
        following = jnp.minimum(t + 1, count - 1)
        making = generate(following, later)
        left = left_of(jnp.maximum(t - 1, 0))
        for k in range(TOP):
            take((k - LAG) % TOP, left)
            if k == LAG - 1:
                left = left_of(t)
            pltpu.matmul_acc_lhs(
                sum_of(k), basis_function(k, now), load_staged_rhs=0 if k < 2 else None
            )
            if k == 8:
                stage(following)
            next(making, None)
        for _ in making:
            pass

    for one in sums[0] + sums[1]:
        pltpu.matmul_pop(one)
    for _ in generate(0, even):
        pass
    stage(0)

    def step(pair, carry):
        process(2 * pair, even, odd)
        process(2 * pair + 1, odd, even)
        return carry

    lax.fori_loop(0, count // 2, step, 0)
    left = left_of(count - 1)
    for k in range(TOP - LAG, TOP):
        take(k, left)
    for unit in range(2):
        pltpu.matmul_acc_lhs(sums[unit][0], jnp.zeros((ROWS, COLS), bf16), load_staged_rhs=0)
        pltpu.matmul_pop(sums[unit][0])

    halves = [jnp.zeros((L // 2, LANES), f32)] * 2
    for k in range(TOP + 1):
        odd_one = PARITY[k]
        column = basis_ref[odd_one, :, k : k + 1]
        halves[odd_one] += column * jnp.sum(total[k], axis=0, keepdims=True)
    for odd_one in range(2):
        out_ref[L // 2 * odd_one : L // 2 * (odd_one + 1)] = halves[odd_one][:, :LANE]
    lane = lax.broadcasted_iota(jnp.int32, (L // 2, LANE), 1)
    upper, lower = halves[0][:, LANE:], halves[1][:, LANE:]
    out_ref[L:] = jnp.where(lane < LANE // 2, upper, pltpu.roll(lower, LANE // 2, 1))


def assemble_kernel(place_ref, half_ref, other_ref, out_ref, scratch):
    r, c = place_ref[0], place_ref[1]
    half = jnp.where(c // 2 > r, c % 2, 1 - c % 2)
    for piece in range(NR):
        at = pl.multiple_of(CHUNK * half + PIECE * piece, PIECE)
        scratch[pl.ds(at, PIECE)] = unpacked(half_ref[piece])
        at = pl.multiple_of(CHUNK * (1 - half) + PIECE * piece, PIECE)
        scratch[pl.ds(at, PIECE)] = unpacked(other_ref[piece])
    out_ref[...] = scratch[...][:, :MAPS].T


def finish_kernel(own_ref, near_ref, far_ref, across_ref, out_ref, scratch):
    value = (own_ref[...] + across_ref[...]) + (near_ref[...] + far_ref[...])
    rest = value[L:]
    for odd_one in range(2):
        rows = value[L // 2 * odd_one : L // 2 * (odd_one + 1)]
        last = pltpu.roll(rest, LANE // 2, 1) if odd_one else rest
        scratch[0, pl.ds(odd_one, L // 2, 2)] = rows
        scratch[1, pl.ds(odd_one, L // 2, 2)] = last
    out_ref[:, :LANE] = scratch[0]
    out_ref[:, LANE:] = scratch[1][:, : MAPS - LANE]


SMEM = pl.BlockSpec(memory_space=pltpu.SMEM)
VMEM = pl.BlockSpec(memory_space=pltpu.VMEM)


def partial_products(cov, maps, cosines):
    tall = LENT * ROWS
    blocks = [
        pl.BlockSpec((tall, COLS), lambda i, first=first: (first // tall, 1))
        for first in (LENT_ROW, CHUNK + LENT_ROW)
    ]
    whole = [pl.BlockSpec(array.shape, lambda i: (0, 0)) for array in (cov, maps)]
    shapes = (NC, SENT, LANE), (2, tall, COLS)
    return pl.pallas_call(
        partial_kernel,
        grid=(1,),
        out_shape=tuple(pltpu.VMEM(shape, f32) for shape in shapes),
        in_specs=whole + blocks,
        out_specs=tuple(pl.BlockSpec(shape, lambda i: (0, 0, 0)) for shape in shapes),
        compiler_params=pltpu.CompilerParams(vmem_limit_bytes=16 * 2**20),
        name="partial",
    )(cov, maps, cosines, cosines)


def block_spectra(place, cosines, lent, rows, cols):
    return pl.pallas_call(
        spectra_kernel,
        out_shape=(pltpu.VMEM((L + L // 2, LANE), f32), pltpu.VMEM((NR, SENT, LANE), bf16)),
        in_specs=[SMEM] + [VMEM] * 11,
        out_specs=(VMEM, VMEM),
        scratch_shapes=[
            pltpu.VMEM((2 * CHUNK, LANES), bf16),
            pltpu.VMEM((CHUNK, LANES), bf16),
            pltpu.VMEM((FACTORS, ROWS, COLS), bf16),
            pltpu.VMEM((FACTORS, ROWS, COLS), bf16),
            pltpu.VMEM((TOP + 1, 8, LANES), f32),
        ],
        cost_estimate=pl.CostEstimate(flops=9 * 10**9, bytes_accessed=4 * 10**6, transcendentals=0),
        compiler_params=pltpu.CompilerParams(
            vmem_limit_bytes=24 * 2**20,
        ),
        name="spectra",
    )(place, cosines, lent, *rows, *cols, jnp.asarray(BASIS))


def assemble(place, half, other):
    return pl.pallas_call(
        assemble_kernel,
        out_shape=jax.ShapeDtypeStruct((MAPS, 2 * CHUNK), bf16),
        in_specs=[SMEM, VMEM, VMEM],
        out_specs=VMEM,
        scratch_shapes=[pltpu.VMEM((2 * CHUNK, LANES), bf16)],
        compiler_params=pltpu.CompilerParams(vmem_limit_bytes=8 * 2**20),
        name="assemble",
    )(place, half, other).T


def finish(*terms):
    return pl.pallas_call(
        finish_kernel,
        out_shape=jax.ShapeDtypeStruct((L, MAPS), f32),
        in_specs=[VMEM] * 4,
        out_specs=VMEM,
        scratch_shapes=[pltpu.VMEM((2, L, LANE), f32)],
        compiler_params=pltpu.CompilerParams(vmem_limit_bytes=4 * 2**20),
        name="finish",
    )(*terms)


def everywhere(value):
    value = value + lax.ppermute(value, PROW[1], [(0, 1), (1, 0)])
    terms = (value,)
    for axis in (PROW[0],) + PCOL:
        if len(terms) > 1:
            value = (terms[0] + terms[3]) + (terms[1] + terms[2])
        terms = (value,) + tuple(
            lax.ppermute(value, axis, [(i, i ^ mask) for i in range(4)]) for mask in (1, 3, 2)
        )
    return terms


def per_device(inverse_cov, cosines, sky_maps):
    place = jnp.stack([lax.axis_index(PROW), lax.axis_index(PCOL)]).astype(jnp.int32)
    inverse_cov, sky_maps, corner = (
        pltpu.with_memory_space_constraint(value, pltpu.HBM)
        for value in (inverse_cov, sky_maps.T, cosines)
    )
    partial, lent = partial_products(inverse_cov, sky_maps, corner)
    partial = partial.astype(f16)
    parts = lax.all_to_all(partial, ALL, 0, 0, axis_index_groups=SUMMERS, tiled=True)
    piece = jnp.sum(parts.astype(f32), axis=0).astype(bf16)
    lent, piece = lax.optimization_barrier((lent, piece))
    lent = lax.ppermute(lent, PROW[1], [(0, 1), (1, 0)])

    cols, rows = lax.ppermute(piece, ALL, TO_COLUMNS)[None], piece[None]
    rows = jnp.concatenate([rows, lax.ppermute(rows, ALL, ROW_STEPS[0])])
    cols = jnp.concatenate([cols, lax.ppermute(cols, ALL, COLUMN_STEPS[0])])
    rows = [rows] + [lax.ppermute(rows, ALL, pairs) for pairs in ROW_STEPS[1:]]
    cols = [cols] + [lax.ppermute(cols, ALL, pairs) for pairs in COLUMN_STEPS[1:]]

    cosines = pltpu.with_memory_space_constraint(cosines, pltpu.VMEM)
    share, half = block_spectra(place, cosines, lent, rows, cols)
    other = lax.ppermute(half, ALL, OTHER_HALF)
    spectra = finish(*everywhere(share))
    return assemble(place, half, other), spectra


def solution(mesh):
    split = Mesh(mesh.devices.reshape(4, 2, 4, 4), ALL)
    placed = (P(PROW, PCOL), P(PROW, PCOL), P(PCOL, None))
    return jax.shard_map(
        per_device, mesh=split, in_specs=placed, out_specs=(P(PROW, None), P()), check_vma=False
    )
```

```python
import functools

import jax
import jax.numpy as jnp
import numpy as np
from jax import lax
from jax.experimental import pallas as pl
from jax.experimental.pallas import tpu as pltpu
from jax.sharding import Mesh
from jax.sharding import PartitionSpec as P

NPIX = 8192
MAPS = 192
L = 64
LMIN = 2
TOP = LMIN + L - 1
NR, NC = 8, 16
CHUNK = NPIX // NC
PIECE = CHUNK // NR
LANES = 256
LANE = 128
SENT = PIECE * MAPS // LANE
ROWS = 32
COLS = 256
LOW = 9
CENTRES = (18, 37, 56)
CENTRE = 2 * LOW - 1
FACTORS = CENTRE + 2 * len(CENTRES)
LENT = 4
LENT_ROW = 256
LAG = 28
PROW = ("prow_0", "prow_1")
PCOL = ("pcol_0", "pcol_1")
ALL = PROW + PCOL
bf16, f16, f32 = jnp.bfloat16, jnp.float16, jnp.float32
MASKS = (1, 2, 6, 4)
ORDER = (0, 1, 2, 3, 6, 7, 4, 5)


def half_of(r, c):
    return c % 2 if c // 2 > r else 1 - c % 2


def keeper_of(g, y):
    return 2 * ((2 * y + 2 - g // 2) % 4) + g % 2


MEMBERS = [
    [[c for c in range(NC) if half_of(r, c) == s] for s in range(2)] for r in range(NR)
]
EACH = [(r, s, g) for r in range(NR) for s in range(2) for g in range(NR)]
TO_COLUMNS = [
    (r * NC + MEMBERS[r][s][g], keeper_of(g, r // 2) * NC + 2 * r + s) for r, s, g in EACH
]
OTHER_HALF = [(r * NC + MEMBERS[r][s][g], r * NC + MEMBERS[r][1 - s][g]) for r, s, g in EACH]
SUMMERS = [[r * NC + MEMBERS[r][s][g] for s in range(2) for g in range(NR)] for r in range(NR)]
ROW_STEPS = [
    [(r * NC + MEMBERS[r][s][g], r * NC + MEMBERS[r][s][g ^ mask]) for r, s, g in EACH]
    for mask in MASKS
]
COLUMN_STEPS = [
    [(r * NC + c, (r ^ mask) * NC + c) for r in range(NR) for c in range(NC)] for mask in MASKS
]


def basis_matrix():
    g = [1.0]
    for k in range(1, TOP + 1):
        g.append(g[-1] * (2 * k - 1) / (2 * k))
    cheb = np.zeros((L, TOP + 1))
    for row in range(L):
        degree = row + LMIN
        for k in range(degree + 1):
            cheb[row, abs(degree - 2 * k)] += g[k] * g[degree - k]
        cheb[row] *= 2.0 * (2.0 * degree + 1.0) / NPIX
    columns = [cheb[:, k] for k in range(LOW)]
    for n in CENTRES:
        columns.append(cheb[:, n])
        columns += [cheb[:, n - a] + cheb[:, n + a] for a in range(1, LOW + 1)]
        columns += [cheb[:, n - a] - cheb[:, n + a] for a in range(1, LOW + 1)]
    matrix = np.stack(columns, axis=1)
    assert matrix.shape == (L, TOP + 1)
    matrix = matrix.reshape(L // 2, 2, TOP + 1).transpose(1, 0, 2).astype(np.float32)
    parity = [int(not matrix[0, :, k].any()) for k in range(TOP + 1)]
    assert all(not matrix[1 - parity[k], :, k].any() for k in range(TOP + 1))
    return matrix, parity


BASIS, PARITY = basis_matrix()


def factors(x):
    y = x + x
    t, u = [jnp.ones_like(x), x], [jnp.ones_like(x), y]
    yield 0, x.astype(bf16)
    yield LOW, y.astype(bf16)
    for k in range(2, LOW + 1):
        t.append(y * t[k - 1] - t[k - 2])
        yield k - 1, t[k].astype(bf16)
        if k < LOW:
            u.append(y * u[k - 1] - u[k - 2])
            yield LOW + k - 1, u[k].astype(bf16)
    t9, u8 = t[9], u[8]
    square = 1.0 - x * x
    double = t9 + t9
    t18, u17 = double * t9 - 1.0, double * u8
    v18 = square * u17
    yield CENTRE, t18.astype(bf16)
    yield CENTRE + 1, v18.astype(bf16)
    double = t18 + t18
    t36, v36 = double * t18 - 1.0, double * v18
    t37, v37 = t36 * x - v36, v36 * x + t36 * square
    yield CENTRE + 2, t37.astype(bf16)
    yield CENTRE + 3, v37.astype(bf16)
    t19, u18 = t18 * x - v18, u17 * x + t18
    v19 = square * u18
    t56, v56 = t37 * t19 - v37 * u18, v37 * t19 + t37 * v19
    yield CENTRE + 4, t56.astype(bf16)
    yield CENTRE + 5, v56.astype(bf16)


def basis_function(k, made):
    if k < LOW - 1:
        return made[k]
    centre, which = divmod(k - (LOW - 1), 2 * LOW + 1)
    tn, vn = CENTRE + 2 * centre, CENTRE + 2 * centre + 1
    if which == 0:
        return made[tn]
    if which <= LOW:
        return made[tn] * made[which - 1]
    if which == LOW + 1:
        return made[vn]
    return made[vn] * made[LOW + which - LOW - 2]


def unpacked(piece):
    rest = piece[PIECE:].astype(f32)
    first = lax.broadcasted_iota(jnp.int32, rest.shape, 1) < LANE // 2
    upper = jnp.where(first, rest, 0.0)
    lower = jnp.where(first, pltpu.roll(rest, LANE // 2, 1), 0.0)
    rest = jnp.concatenate([upper, lower], axis=0).astype(piece.dtype)
    return jnp.concatenate([piece[:PIECE], rest], axis=1)


def partial_kernel(cov_ref, maps_ref, upper_ref, lower_ref, out_ref, lent_ref):
    lent_ref[0] = upper_ref[...]
    lent_ref[1] = lower_ref[...]
    zeros = jnp.zeros((LANES - MAPS, maps_ref.shape[1]), bf16)
    maps = jnp.concatenate([maps_ref[...], zeros], axis=0)
    product = lax.dot_general(
        cov_ref[...], maps, (((1,), (1,)), ((), ())), preferred_element_type=f32
    )
    for piece in range(NC):
        rows = product[PIECE * piece : PIECE * (piece + 1)]
        out_ref[piece, :PIECE] = rows[:, :LANE]
        rest = rows[:, LANE:]
        out_ref[piece, PIECE:] = rest[: PIECE // 2] + pltpu.roll(rest[PIECE // 2 :], LANE // 2, 1)


def spectra_kernel(
    place_ref, cos_ref, lent_ref, r0, r1, r2, r3, c0, c1, c2, c3, basis_ref, out_ref, half_ref,
    maps, weights, even, odd, total,
):
    def with_sums(*sums):
        spectra_body(
            place_ref, cos_ref, lent_ref, (r0, r1, r2, r3), (c0, c1, c2, c3), basis_ref, out_ref, half_ref,
            maps, weights, even, odd, total, (sums[:17], sums[17:]),
        )

    pl.run_scoped(
        with_sums,
        *[pltpu.ACC(0)((ROWS, LANES), f32)] * 17,
        *[pltpu.ACC(1)((ROWS, LANES), f32)] * 16,
    )


def pieces_of(refs):
    return [(ref, at) for ref in refs for at in range(ref.shape[0])]


def spectra_body(
    place_ref, cos_ref, lent_ref, rows_refs, cols_refs, basis_ref, out_ref, half_ref,
    maps, weights, even, odd, total, sums,
):
    r, c = place_ref[0], place_ref[1]
    group, own = c // 2, c % 2
    other = 1 - own
    diagonal = group == r
    half = jnp.where(group > r, own, other)
    row_sum = col_sum = jnp.zeros((8, LANES), f32)
    for order, (rows_ref, at), (cols_ref, _) in zip(ORDER, pieces_of(rows_refs), pieces_of(cols_refs)):
        rows = unpacked(rows_ref[at])
        to = pl.multiple_of((group ^ order) * PIECE, PIECE)
        maps[pl.ds(to, PIECE)] = rows
        half_ref[group ^ order] = rows_ref[at]
        cols = unpacked(cols_ref[at])
        to = pl.multiple_of(keeper_of(r ^ order, c // 4) * PIECE, PIECE)
        weights[pl.ds(to, PIECE)] = cols
        maps[pl.ds(CHUNK + to, PIECE)] = cols
        row_sum += jnp.sum(rows.astype(f32).reshape(PIECE // 8, 8, LANES), axis=0)
        col_sum += jnp.sum(cols.astype(f32).reshape(PIECE // 8, 8, LANES), axis=0)
    row_sum = jnp.sum(row_sum, axis=0, keepdims=True)
    col_sum = jnp.sum(col_sum, axis=0, keepdims=True)
    alpha = jnp.where(diagonal, 0.5, 1.0)
    beta = jnp.where(diagonal, 0.5, 0.0)
    total[...] = jnp.zeros_like(total)
    total[0, 0:1] = col_sum * (alpha * row_sum + beta * col_sum)
    helper = group == r ^ 1
    count = jnp.where(jnp.logical_or(diagonal, helper), 32 + LENT, 32)

    def tile(t):
        part, first = t // 8, 32 * (t % 8)
        plain_row = 32 * (t % 16)
        lent = jnp.logical_and(helper, t >= 32)
        plain = (
            jnp.where(lent, 32 * (t - 32), CHUNK * half + plain_row),
            jnp.where(lent, LENT_ROW + CHUNK + 32 * (t - 32), plain_row),
            jnp.where(lent, 1, t // 16),
            jnp.where(lent, 0.5, 1.0),
        )
        kept = jnp.where(t >= 16, t + LENT, t)
        part, first = kept // 8, 32 * (kept % 8)
        mine = part < 3
        low = jnp.logical_or(part == 2, jnp.logical_and(part == 4, own == 1))
        row = first + jnp.where(low, LENT_ROW, 0)
        column = jnp.where(mine, jnp.minimum(part, 1), jnp.where(part == 3, own, 1))
        weight = jnp.where(jnp.logical_or(part == 0, part == 2), 0.5, 1.0)
        chosen = (
            CHUNK * jnp.where(mine, own, other) + row,
            CHUNK * jnp.where(mine, 1, 0) + row,
            column,
            weight,
        )
        return [jnp.where(diagonal, a, b) for a, b in zip(chosen, plain)] + [lent]

    def generate(t, slot):
        cos_row, _, column, _, lent = tile(t)
        cos_row = pl.multiple_of(cos_row, ROWS)
        lent_row = pl.multiple_of(jnp.where(lent, cos_row, 0), ROWS)
        column = pl.multiple_of(column * COLS, COLS)
        for first in range(0, ROWS, 16):
            x = cos_ref[pl.ds(cos_row + first, 16), pl.ds(column, COLS)]
            x = jnp.where(lent, lent_ref[own, pl.ds(lent_row + first, 16)], x)
            for which, value in factors(x):
                slot[which, first : first + 16] = value
                yield

    def stage(t):
        column = tile(t)[2]
        right = weights[pl.ds(pl.multiple_of(column * COLS, COLS), COLS)]
        for unit in range(2):
            pltpu.matmul_push_rhs(right, 0, unit)

    def left_of(t):
        _, map_row, _, weight, _ = tile(t)
        return maps[pl.ds(pl.multiple_of(map_row, ROWS), ROWS)].astype(f32) * weight

    def sum_of(k):
        unit, turn = k % 2, k // 2
        return sums[unit][turn % 16 if turn < 32 else 16]

    def take(k, left):
        product = pltpu.matmul_pop(sum_of(k)) * left
        total[k + 1] += jnp.sum(product.reshape(ROWS // 8, 8, LANES), axis=0)

    def process(t, now, later):
        following = jnp.minimum(t + 1, count - 1)
        making = generate(following, later)
        left = left_of(jnp.maximum(t - 1, 0))
        for k in range(TOP):
            take((k - LAG) % TOP, left)
            if k == LAG - 1:
                left = left_of(t)
            pltpu.matmul_acc_lhs(
                sum_of(k), basis_function(k, now), load_staged_rhs=0 if k < 2 else None
            )
            if k == 8:
                stage(following)
            next(making, None)
        for _ in making:
            pass

    for one in sums[0] + sums[1]:
        pltpu.matmul_pop(one)
    for _ in generate(0, even):
        pass
    stage(0)

    def step(pair, carry):
        process(2 * pair, even, odd)
        process(2 * pair + 1, odd, even)
        return carry

    lax.fori_loop(0, count // 2, step, 0)
    left = left_of(count - 1)
    for k in range(TOP - LAG, TOP):
        take(k, left)
    for unit in range(2):
        pltpu.matmul_acc_lhs(sums[unit][0], jnp.zeros((ROWS, COLS), bf16), load_staged_rhs=0)
        pltpu.matmul_pop(sums[unit][0])

    halves = [jnp.zeros((L // 2, LANES), f32)] * 2
    for k in range(TOP + 1):
        odd_one = PARITY[k]
        column = basis_ref[odd_one, :, k : k + 1]
        halves[odd_one] += column * jnp.sum(total[k], axis=0, keepdims=True)
    for odd_one in range(2):
        out_ref[L // 2 * odd_one : L // 2 * (odd_one + 1)] = halves[odd_one][:, :LANE]
    lane = lax.broadcasted_iota(jnp.int32, (L // 2, LANE), 1)
    upper, lower = halves[0][:, LANE:], halves[1][:, LANE:]
    out_ref[L:] = jnp.where(lane < LANE // 2, upper, pltpu.roll(lower, LANE // 2, 1))


def assemble_kernel(place_ref, half_ref, other_ref, out_ref, scratch):
    r, c = place_ref[0], place_ref[1]
    half = jnp.where(c // 2 > r, c % 2, 1 - c % 2)
    for piece in range(NR):
        at = pl.multiple_of(CHUNK * half + PIECE * piece, PIECE)
        scratch[pl.ds(at, PIECE)] = unpacked(half_ref[piece])
        at = pl.multiple_of(CHUNK * (1 - half) + PIECE * piece, PIECE)
        scratch[pl.ds(at, PIECE)] = unpacked(other_ref[piece])
    out_ref[...] = scratch[...][:, :MAPS].T


def finish_kernel(own_ref, near_ref, far_ref, across_ref, out_ref, scratch):
    value = (own_ref[...] + across_ref[...]) + (near_ref[...] + far_ref[...])
    rest = value[L:]
    for odd_one in range(2):
        rows = value[L // 2 * odd_one : L // 2 * (odd_one + 1)]
        last = pltpu.roll(rest, LANE // 2, 1) if odd_one else rest
        scratch[0, pl.ds(odd_one, L // 2, 2)] = rows
        scratch[1, pl.ds(odd_one, L // 2, 2)] = last
    out_ref[:, :LANE] = scratch[0]
    out_ref[:, LANE:] = scratch[1][:, : MAPS - LANE]


SMEM = pl.BlockSpec(memory_space=pltpu.SMEM)
VMEM = pl.BlockSpec(memory_space=pltpu.VMEM)


def partial_products(cov, maps, cosines):
    tall = LENT * ROWS
    blocks = [
        pl.BlockSpec((tall, COLS), lambda i, first=first: (first // tall, 1))
        for first in (LENT_ROW, CHUNK + LENT_ROW)
    ]
    whole = [pl.BlockSpec(array.shape, lambda i: (0, 0)) for array in (cov, maps)]
    shapes = (NC, SENT, LANE), (2, tall, COLS)
    return pl.pallas_call(
        partial_kernel,
        grid=(1,),
        out_shape=tuple(pltpu.VMEM(shape, f32) for shape in shapes),
        in_specs=whole + blocks,
        out_specs=tuple(pl.BlockSpec(shape, lambda i: (0, 0, 0)) for shape in shapes),
        compiler_params=pltpu.CompilerParams(vmem_limit_bytes=16 * 2**20),
        name="partial",
    )(cov, maps, cosines, cosines)


def block_spectra(place, cosines, lent, rows, cols):
    return pl.pallas_call(
        spectra_kernel,
        out_shape=(pltpu.VMEM((L + L // 2, LANE), f32), pltpu.VMEM((NR, SENT, LANE), bf16)),
        in_specs=[SMEM] + [VMEM] * 11,
        out_specs=(VMEM, VMEM),
        scratch_shapes=[
            pltpu.VMEM((2 * CHUNK, LANES), bf16),
            pltpu.VMEM((CHUNK, LANES), bf16),
            pltpu.VMEM((FACTORS, ROWS, COLS), bf16),
            pltpu.VMEM((FACTORS, ROWS, COLS), bf16),
            pltpu.VMEM((TOP + 1, 8, LANES), f32),
        ],
        cost_estimate=pl.CostEstimate(flops=9 * 10**9, bytes_accessed=4 * 10**6, transcendentals=0),
        compiler_params=pltpu.CompilerParams(
            vmem_limit_bytes=24 * 2**20,
        ),
        name="spectra",
    )(place, cosines, lent, *rows, *cols, jnp.asarray(BASIS))


def assemble(place, half, other):
    return pl.pallas_call(
        assemble_kernel,
        out_shape=jax.ShapeDtypeStruct((MAPS, 2 * CHUNK), bf16),
        in_specs=[SMEM, VMEM, VMEM],
        out_specs=VMEM,
        scratch_shapes=[pltpu.VMEM((2 * CHUNK, LANES), bf16)],
        compiler_params=pltpu.CompilerParams(vmem_limit_bytes=8 * 2**20),
        name="assemble",
    )(place, half, other).T


def finish(*terms):
    return pl.pallas_call(
        finish_kernel,
        out_shape=jax.ShapeDtypeStruct((L, MAPS), f32),
        in_specs=[VMEM] * 4,
        out_specs=VMEM,
        scratch_shapes=[pltpu.VMEM((2, L, LANE), f32)],
        compiler_params=pltpu.CompilerParams(vmem_limit_bytes=4 * 2**20),
        name="finish",
    )(*terms)


def everywhere(value):
    value = value + lax.ppermute(value, PROW[1], [(0, 1), (1, 0)])
    terms = (value,)
    for axis in (PCOL[1], PCOL[0], PROW[0]):
        if len(terms) > 1:
            value = (terms[0] + terms[3]) + (terms[1] + terms[2])
        terms = (value,) + tuple(
            lax.ppermute(value, axis, [(i, i ^ mask) for i in range(4)]) for mask in (1, 3, 2)
        )
    return terms


def per_device(inverse_cov, cosines, sky_maps):
    place = jnp.stack([lax.axis_index(PROW), lax.axis_index(PCOL)]).astype(jnp.int32)
    inverse_cov, sky_maps, corner = (
        pltpu.with_memory_space_constraint(value, pltpu.HBM)
        for value in (inverse_cov, sky_maps.T, cosines)
    )
    partial, lent = partial_products(inverse_cov, sky_maps, corner)
    partial = partial.astype(f16)
    parts = lax.all_to_all(partial, ALL, 0, 0, axis_index_groups=SUMMERS, tiled=True)
    piece = jnp.sum(parts.astype(f32), axis=0).astype(bf16)
    lent, piece = lax.optimization_barrier((lent, piece))
    lent = lax.ppermute(lent, PROW[1], [(0, 1), (1, 0)])

    cols, rows = lax.ppermute(piece, ALL, TO_COLUMNS)[None], piece[None]
    rows = jnp.concatenate([rows, lax.ppermute(rows, ALL, ROW_STEPS[0])])
    cols = jnp.concatenate([cols, lax.ppermute(cols, ALL, COLUMN_STEPS[0])])
    rows = [rows] + [lax.ppermute(rows, ALL, pairs) for pairs in ROW_STEPS[1:]]
    cols = [cols] + [lax.ppermute(cols, ALL, pairs) for pairs in COLUMN_STEPS[1:]]

    cosines = pltpu.with_memory_space_constraint(cosines, pltpu.VMEM)
    share, half = block_spectra(place, cosines, lent, rows, cols)
    other = lax.ppermute(half, ALL, OTHER_HALF)
    spectra = finish(*everywhere(share))
    return assemble(place, half, other), spectra


def solution(mesh):
    split = Mesh(mesh.devices.reshape(4, 2, 4, 4), ALL)
    placed = (P(PROW, PCOL), P(PROW, PCOL), P(PCOL, None))
    return jax.shard_map(
        per_device, mesh=split, in_specs=placed, out_specs=(P(PROW, None), P()), check_vma=False
    )
```
